8 devices in a mesh: depth: 2 (over z, y), col: 2 (over x), row: 2 (over core).
Axes of the slice: x: 2, y: 2, z: 1, core: 2. Of those that a mesh axis runs over, the one named last changes fastest.
Arguments:
- weight: bfloat16 [6144, 6144], P(('row', 'depth'), 'col')
- rhs_stack: bfloat16 [3, 6144, 4096], P(None, ('row', 'depth'), 'col')
Outputs:
- output: bfloat16 [3, 6144, 4096], P(None, ('row', 'depth'), 'col')
All inputs are finite; a program needn't handle non-finite values.
Results may differ from the reference program's by a relative error of at most 0.001.
Values are sent between devices in bfloat16 or wider.
A program may use at most 1 GiB of HBM per device.

```python
import jax
import jax.numpy as jnp
from jax import lax

N = 6144
RHS_COLS = 4096


def setup_inputs(seed: int = 0) -> dict:
    base_key = jax.random.key(seed)
    key_w, key_x = jax.random.split(base_key)
    weight = jax.random.normal(key_w, (N, N), jnp.float32) * (N ** -0.5) + 2.0 / N
    rhs_stack = jax.random.normal(key_x, (3, N, RHS_COLS), jnp.float32) + 0.5
    return {"weight": weight.astype(jnp.bfloat16), "rhs_stack": rhs_stack.astype(jnp.bfloat16)}


def reference(weight, rhs_stack):
    def one_product(rhs_block):
        return jnp.dot(weight, rhs_block, preferred_element_type=jnp.float32).astype(jnp.bfloat16)
    return lax.map(one_product, rhs_stack)
```

```python
import functools

import jax
import jax.numpy as jnp
from jax import lax
from jax.experimental import pallas as pl
from jax.experimental.pallas import tpu as pltpu
from jax.sharding import PartitionSpec as P


SWAP = [(0, 1), (1, 0)]
CHUNKS = (
    (0, 0, 512, 0, 1536),
    (0, 512, 1536, 0, 1536),
    (1, 0, 1024, 0, 1536),
    (1, 1024, 1024, 0, 1536),
    (2, 0, 512, 0, 1536),
    (2, 512, 512, 0, 1536),
    (2, 1024, 512, 0, 1536),
    (2, 1536, 256, 0, 1536),
    (2, 1792, 256, 0, 768),
    (2, 1792, 256, 768, 768),
)
LATE = 4
TAIL = 8
TILE_ROWS = 512
TILE_COLS = 512


def product_kernel(plan, *refs):
    tiles, flips, windows, k_start, k_rows, has_base, has_prev, width, tile_cols = plan
    n_tiles, n_pieces = len(tiles), len(flips)
    a_own, a_far = refs[0], refs[1 : 1 + n_tiles]
    pieces = refs[1 + n_tiles : 1 + n_tiles + n_pieces]
    rest = refs[1 + n_tiles + n_pieces :]
    base_ref = rest[0] if has_base else None
    out_ref, a_all, x_all, a_sems, x_sems = rest[has_base + has_prev :]
    slice_rows = a_own.shape[1] // 2
    layer_idx = lax.axis_index("depth")
    cross = lax.rem(lax.axis_index("col") + lax.axis_index("row"), 2)
    m, n = pl.program_id(0), pl.program_id(1)
    layers = sorted({flip_layer for _, flip_layer in flips})
    n_layers = len(layers)
    col_tiles = width // tile_cols

    def a_copy(side, tile):
        if side == 0:
            source = a_own.at[pl.ds(tiles[tile] * TILE_ROWS, TILE_ROWS)]
        else:
            source = a_far[tile]
        if n_layers == 1:
            start = lax.rem(layer_idx + layers[0], 2) * slice_rows + k_start
            source = source.at[:, pl.ds(pl.multiple_of(start, 128), k_rows)]
        return pltpu.make_async_copy(source, a_all.at[side, pl.ds(tile * TILE_ROWS, TILE_ROWS)], a_sems.at[side, tile])

    def x_copy(idx, tile):
        flip_row, flip_layer = flips[idx]
        slot = lax.rem(cross + flip_row, 2) * n_layers
        if n_layers == 2:
            slot = slot + lax.rem(layer_idx + flip_layer, 2)
        source = pieces[idx]
        start = tile * tile_cols
        if windows[idx] is not None:
            rhs_idx, offset = windows[idx]
            source = source.at[rhs_idx]
            start = start + offset
        return pltpu.make_async_copy(
            source.at[:, pl.ds(start, tile_cols)],
            x_all.at[slot, :, pl.ds(tile * tile_cols, tile_cols)],
            x_sems.at[slot, tile],
        )

    def x_wait(side, tile):
        for layer in range(n_layers):
            slot = side * n_layers + layer
            block = x_all.at[slot, :, pl.ds(tile * tile_cols, tile_cols)]
            pltpu.make_async_copy(block, block, x_sems.at[slot, tile]).wait()

    def x_start(side, tile):
        for idx, (flip_row, _) in enumerate(flips):
            @pl.when(lax.rem(cross + flip_row, 2) == side)
            def _():
                x_copy(idx, tile).start()

    groups = [(0, col, side) for col in range(col_tiles) for side in range(2)]
    groups += [(tile, 0, side) for tile in range(1, n_tiles) for side in range(2)]

    def group_start(index):
        if index < len(groups):
            tile, col, side = groups[index]
            if col == 0:
                a_copy(side, tile).start()
            if tile == 0:
                x_start(side, col)

    def group_wait(index):
        tile, col, side = groups[index]
        if col == 0:
            a_copy(side, tile).wait()
        if tile == 0:
            x_wait(side, col)

    row_range = pl.ds(pl.multiple_of(m * TILE_ROWS, TILE_ROWS), TILE_ROWS)
    col_range = pl.ds(pl.multiple_of(n * tile_cols, tile_cols), tile_cols)
    total = base_ref[...] if has_base else None
    for side in range(2):
        for index, (tile, col, group_side) in enumerate(groups):
            if group_side == side:
                @pl.when((m == tile) & (n == col))
                def _():
                    if index == 0:
                        group_start(0)
                    group_wait(index)
                    if index == 0:
                        group_start(1)
                    group_start(index + 2)

        x_side = x_all[pl.ds(side * n_layers, n_layers), :, col_range].reshape(n_layers * k_rows, tile_cols)
        term = jnp.dot(a_all[side, row_range], x_side, preferred_element_type=jnp.float32)
        total = term if total is None else total + term
    if len(out_ref.shape) == 3:
        out_ref[0] = total.astype(out_ref.dtype)
    else:
        out_ref[...] = total


def product(a_own, a_far, pieces, flips, windows, k_range, width, tiles=(0, 1, 2), base=None, base_start=0, prev=None, out=None):
    rows, half = a_own.shape
    k_start, k_rows = k_range
    any_spec = pl.BlockSpec(memory_space=pl.ANY)
    tile_cols = min(TILE_COLS, width)
    n_layers = len({flip_layer for _, flip_layer in flips})
    operands = [a_own, *(a_far[tile] for tile in tiles), *pieces]
    in_specs = [any_spec] * len(operands)
    first = tiles[0]
    if base is not None:
        operands.append(base)
        in_specs.append(pl.BlockSpec((TILE_ROWS, tile_cols), lambda m, n: (first + m, base_start // tile_cols + n)))
    aliases = {}
    if prev is not None:
        aliases = {len(operands): 0}
        operands.append(prev)
        in_specs.append(any_spec)
    if out is None:
        out_shape = jax.ShapeDtypeStruct((rows, width), jnp.float32)
        out_spec = pl.BlockSpec((TILE_ROWS, tile_cols), lambda m, n: (first + m, n))
    else:
        y_shape, rhs_idx, start = out
        out_shape = jax.ShapeDtypeStruct(y_shape, jnp.bfloat16)
        out_spec = pl.BlockSpec((1, TILE_ROWS, tile_cols), lambda m, n: (rhs_idx, first + m, start // tile_cols + n))
    plan = (tuple(tiles), tuple(flips), tuple(windows), k_start, k_rows, base is not None, prev is not None, width, tile_cols)
    tile_rows = len(tiles) * TILE_ROWS
    vmem = 4 * n_layers * k_rows * (tile_rows + width) + 16 * TILE_ROWS * tile_cols + (8 << 20)
    return pl.pallas_call(
        functools.partial(product_kernel, plan),
        grid=(len(tiles), width // tile_cols),
        out_shape=out_shape,
        in_specs=in_specs,
        out_specs=out_spec,
        scratch_shapes=[
            pltpu.VMEM((2, tile_rows, n_layers * k_rows), jnp.bfloat16),
            pltpu.VMEM((2 * n_layers, k_rows, width), jnp.bfloat16),
            pltpu.SemaphoreType.DMA((2, len(tiles))),
            pltpu.SemaphoreType.DMA((2 * n_layers, width // tile_cols)),
        ],
        input_output_aliases=aliases,
        cost_estimate=pl.CostEstimate(flops=4 * tile_rows * n_layers * k_rows * width, bytes_accessed=4 * tile_rows * half, transcendentals=0),
        compiler_params=pltpu.CompilerParams(dimension_semantics=("arbitrary", "arbitrary"), vmem_limit_bytes=vmem),
        name="product",
    )(*operands)


def tail_kernel(target, *refs):
    a_deep, a_both, x_deep, x_both, base = refs[:5]
    rest = refs[5:]
    total = base[...] + jnp.dot(a_deep[...], x_deep[...], preferred_element_type=jnp.float32)
    total = total + jnp.dot(a_both[...], x_both[...], preferred_element_type=jnp.float32)
    if target is None:
        rest[0][...] = total
        return
    y_ref, stage, sem = rest[1:]
    rhs_idx, start = target
    stage[...] = total.astype(stage.dtype)
    copy = pltpu.make_async_copy(stage, y_ref.at[rhs_idx, :, pl.ds(start, stage.shape[1])], sem)
    copy.start()
    copy.wait()


def tail_product(a_deep, a_both, x_deep, x_both, base, prev=None, target=None):
    vmem_spec = pl.BlockSpec(memory_space=pltpu.VMEM)
    any_spec = pl.BlockSpec(memory_space=pl.ANY)
    operands = [a_deep, a_both, x_deep, x_both, base]
    in_specs = [vmem_spec] * 5
    common = dict(name="tail", compiler_params=pltpu.CompilerParams(vmem_limit_bytes=24 << 20), cost_estimate=pl.CostEstimate(flops=4 * a_deep.size * x_deep.shape[1], bytes_accessed=4 * a_deep.size, transcendentals=0))
    if target is None:
        return pl.pallas_call(functools.partial(tail_kernel, None), out_shape=jax.ShapeDtypeStruct(base.shape, base.dtype), in_specs=in_specs, out_specs=vmem_spec, **common)(*operands)
    return pl.pallas_call(
        functools.partial(tail_kernel, target),
        out_shape=jax.ShapeDtypeStruct(prev.shape, prev.dtype),
        in_specs=in_specs + [any_spec],
        out_specs=any_spec,
        scratch_shapes=[pltpu.VMEM(base.shape, jnp.bfloat16), pltpu.SemaphoreType.DMA],
        input_output_aliases={5: 0},
        **common,
    )(*operands, prev)


OWN, DEEP, PEER, BOTH = (0, 0), (0, 1), (1, 0), (1, 1)


def solution(mesh):
    def permute(value, axis):
        return lax.ppermute(value, axis, SWAP)

    def body(w_local, x_local):
        y_shape = x_local.shape
        slice_rows = y_shape[1]
        n_row_tiles = w_local.shape[0] // TILE_ROWS

        def piece_of(x, chunk):
            rhs_idx, start, width, k_start, k_rows = chunk
            return x[rhs_idx, k_start : k_start + k_rows, start : start + width]

        first = piece_of(x_local, CHUNKS[0])
        first, x_rest, w_rest = lax.optimization_barrier((first, x_local, w_local))
        w_first, w_rest = lax.optimization_barrier((w_rest[:TILE_ROWS], w_rest))
        sends = [first] + [piece_of(x_rest, chunk) for chunk in CHUNKS[1:]]
        deep = [permute(piece, "depth") for piece in sends]
        w_sends = [w_first] + [w_rest[tile * TILE_ROWS : (tile + 1) * TILE_ROWS] for tile in range(1, n_row_tiles)]
        w_far = [permute(piece, "col") for piece in w_sends]
        x_row = permute(x_rest, "row")

        def full(idx, relay, y, tiles):
            rhs_idx, start, width, _, _ = CHUNKS[idx]
            window = (rhs_idx, start)
            return product(w_local, w_far, (x_local, deep[idx], x_row, relay), (OWN, DEEP, PEER, BOTH), (window, None, window, None), (0, slice_rows), width, tiles=tiles, prev=y, out=(y_shape, rhs_idx, start))

        def local(y, x_row, rhs_idx, start, width, tiles, prev=None):
            x_row, y = lax.optimization_barrier((x_row, y))
            window = (rhs_idx, start)
            base = product(w_local, w_far, (x_local, x_row), (OWN, PEER), (window, window), (0, slice_rows), width, tiles=tiles, prev=prev)
            return lax.optimization_barrier((y, base))

        late_rhs, late_start = CHUNKS[LATE][0], CHUNKS[LATE][1]
        main_width = sum(chunk[2] for chunk in CHUNKS[LATE : TAIL - 1])

        relay0 = permute(deep[0], "row")
        y = full(0, relay0, None, (0,))
        y, base = local(y, x_row, late_rhs, late_start, main_width, (0,))
        y = full(0, relay0, y, (1,))
        piece, y = lax.optimization_barrier((deep[1], y))
        relay1 = permute(piece, "row")
        y = full(1, relay1, y, (0, 1))
        y, base = local(y, x_row, late_rhs, late_start, main_width, (1,), prev=base)
        y = full(0, relay0, y, (2,))
        y = full(1, relay1, y, (2,))
        layer_idx = lax.axis_index("depth")
        cross = lax.rem(lax.axis_index("col") + lax.axis_index("row"), 2)

        def tail_weight(flip_row, k_start, k_rows):
            start = lax.rem(layer_idx + 1, 2) * slice_rows + k_start
            own = lax.dynamic_slice_in_dim(w_local, start, k_rows, axis=1)
            far = jnp.concatenate([lax.dynamic_slice_in_dim(tile, start, k_rows, axis=1) for tile in w_far], axis=0)
            return jnp.where(lax.rem(cross + flip_row, 2) == 0, own, far)

        tail_weights = None
        for idx in range(2, len(CHUNKS)):
            rhs_idx, start, width, _, _ = CHUNKS[idx]
            piece, y = lax.optimization_barrier((deep[idx], y))
            relay = permute(piece, "row")
            if idx < LATE:
                y = full(idx, relay, y, (0, 1, 2))
            elif idx < TAIL:
                part, offset = (base, start - late_start) if idx < TAIL - 1 else (base_last, 0)
                y = product(w_local, w_far, (piece, relay), (DEEP, BOTH), (None, None), (0, slice_rows), width, base=part, base_start=offset, prev=y, out=(y_shape, rhs_idx, start))
            elif idx < len(CHUNKS) - 1:
                base_tail = tail_product(*tail_weights[idx - TAIL], piece, relay, base_tail)
            else:
                y = tail_product(*tail_weights[idx - TAIL], piece, relay, base_tail, prev=y, target=(rhs_idx, start))
            if idx == LATE - 1:
                y, base = local(y, x_row, late_rhs, late_start, main_width, (2,), prev=base)
            if idx == LATE:
                for rhs_idx, start, width, _, _ in (CHUNKS[TAIL - 1], CHUNKS[TAIL]):
                    y, part = local(y, x_row, rhs_idx, start, width, (0, 1, 2))
                    base_last, base_tail = (part, None) if start == CHUNKS[TAIL - 1][1] else (base_last, part)
            if idx == TAIL - 3:
                tail_weights = [(tail_weight(0, *chunk[3:]), tail_weight(1, *chunk[3:])) for chunk in CHUNKS[TAIL:]]
                y, tail_weights = lax.optimization_barrier((y, tail_weights))
        return y

    return jax.shard_map(body, mesh=mesh, in_specs=(P(("row", "depth"), "col"), P(None, ("row", "depth"), "col")), out_specs=P(None, ("row", "depth"), "col"), check_vma=False)
```

```python
import functools

import jax
import jax.numpy as jnp
from jax import lax
from jax.experimental import pallas as pl
from jax.experimental.pallas import tpu as pltpu
from jax.sharding import PartitionSpec as P


SWAP = [(0, 1), (1, 0)]
CHUNKS = (
    (0, 0, 512, 0, 1536),
    (0, 512, 1536, 0, 1536),
    (1, 0, 1024, 0, 1536),
    (1, 1024, 1024, 0, 1536),
    (2, 0, 512, 0, 1536),
    (2, 512, 512, 0, 1536),
    (2, 1024, 512, 0, 1536),
    (2, 1536, 256, 0, 1536),
    (2, 1792, 256, 768, 768),
    (2, 1792, 256, 0, 768),
)
SEND_ORDER = (9, 0, 1, 2, 3, 4, 5, 6, 7, 8)
LATE = 4
TILE_ROWS = 512
TILE_COLS = 512
LOCAL_VMEM = 58 << 20


def product_kernel(plan, *refs):
    tiles, flips, windows, k_start, k_rows, has_base, has_prev, width, tile_cols = plan
    n_tiles, n_pieces = len(tiles), len(flips)
    a_own, a_far = refs[0], refs[1 : 1 + n_tiles]
    pieces = refs[1 + n_tiles : 1 + n_tiles + n_pieces]
    rest = refs[1 + n_tiles + n_pieces :]
    base_ref = rest[0] if has_base else None
    out_ref, a_all, x_all, a_sems, x_sems = rest[has_base + has_prev :]
    slice_rows = a_own.shape[1] // 2
    layer_idx = lax.axis_index("depth")
    cross = lax.rem(lax.axis_index("col") + lax.axis_index("row"), 2)
    m, n = pl.program_id(0), pl.program_id(1)
    layers = sorted({flip_layer for _, flip_layer in flips})
    n_layers = len(layers)
    col_tiles = width // tile_cols

    def a_copy(side, tile):
        if side == 0:
            source = a_own.at[pl.ds(tiles[tile] * TILE_ROWS, TILE_ROWS)]
        else:
            source = a_far[tile]
        if n_layers == 1:
            start = lax.rem(layer_idx + layers[0], 2) * slice_rows + k_start
            source = source.at[:, pl.ds(pl.multiple_of(start, 128), k_rows)]
        return pltpu.make_async_copy(source, a_all.at[side, pl.ds(tile * TILE_ROWS, TILE_ROWS)], a_sems.at[side, tile])

    def x_copy(idx, tile):
        flip_row, flip_layer = flips[idx]
        slot = lax.rem(cross + flip_row, 2) * n_layers
        if n_layers == 2:
            slot = slot + lax.rem(layer_idx + flip_layer, 2)
        source = pieces[idx]
        start = tile * tile_cols
        if windows[idx] is not None:
            rhs_idx, offset = windows[idx]
            source = source.at[rhs_idx]
            start = start + offset
        return pltpu.make_async_copy(
            source.at[:, pl.ds(start, tile_cols)],
            x_all.at[slot, :, pl.ds(tile * tile_cols, tile_cols)],
            x_sems.at[slot, tile],
        )

    def x_wait(side, tile):
        for layer in range(n_layers):
            slot = side * n_layers + layer
            block = x_all.at[slot, :, pl.ds(tile * tile_cols, tile_cols)]
            pltpu.make_async_copy(block, block, x_sems.at[slot, tile]).wait()

    def x_start(side, tile):
        for idx, (flip_row, _) in enumerate(flips):
            @pl.when(lax.rem(cross + flip_row, 2) == side)
            def _():
                x_copy(idx, tile).start()

    groups = [(0, col, side) for col in range(col_tiles) for side in range(2)]
    groups += [(tile, 0, side) for tile in range(1, n_tiles) for side in range(2)]

    def group_start(index):
        if index < len(groups):
            tile, col, side = groups[index]
            if col == 0:
                a_copy(side, tile).start()
            if tile == 0:
                x_start(side, col)

    def group_wait(index):
        tile, col, side = groups[index]
        if col == 0:
            a_copy(side, tile).wait()
        if tile == 0:
            x_wait(side, col)

    row_range = pl.ds(pl.multiple_of(m * TILE_ROWS, TILE_ROWS), TILE_ROWS)
    col_range = pl.ds(pl.multiple_of(n * tile_cols, tile_cols), tile_cols)
    total = base_ref[...] if has_base else None
    for side in range(2):
        for index, (tile, col, group_side) in enumerate(groups):
            if group_side == side:
                @pl.when((m == tile) & (n == col))
                def _():
                    if index == 0:
                        group_start(0)
                    group_wait(index)
                    if index == 0:
                        group_start(1)
                    group_start(index + 2)

        x_side = x_all[pl.ds(side * n_layers, n_layers), :, col_range].reshape(n_layers * k_rows, tile_cols)
        term = jnp.dot(a_all[side, row_range], x_side, preferred_element_type=jnp.float32)
        total = term if total is None else total + term
    if len(out_ref.shape) == 3:
        out_ref[0] = total.astype(out_ref.dtype)
    else:
        out_ref[...] = total


def product(a_own, a_far, pieces, flips, windows, k_range, width, tiles=(0, 1, 2), vmem=None, base=None, base_start=0, prev=None, out=None):
    rows, half = a_own.shape
    k_start, k_rows = k_range
    any_spec = pl.BlockSpec(memory_space=pl.ANY)
    tile_cols = min(TILE_COLS, width)
    n_layers = len({flip_layer for _, flip_layer in flips})
    operands = [a_own, *(a_far[tile] for tile in tiles), *pieces]
    in_specs = [any_spec] * len(operands)
    first = tiles[0]
    if base is not None:
        operands.append(base)
        in_specs.append(pl.BlockSpec((TILE_ROWS, tile_cols), lambda m, n: (first + m, base_start // tile_cols + n)))
    aliases = {}
    if prev is not None:
        aliases = {len(operands): 0}
        operands.append(prev)
        in_specs.append(any_spec)
    if out is None:
        out_shape = jax.ShapeDtypeStruct((rows, width), jnp.float32)
        out_spec = pl.BlockSpec((TILE_ROWS, tile_cols), lambda m, n: (first + m, n))
    else:
        y_shape, rhs_idx, start = out
        out_shape = jax.ShapeDtypeStruct(y_shape, jnp.bfloat16)
        out_spec = pl.BlockSpec((1, TILE_ROWS, tile_cols), lambda m, n: (rhs_idx, first + m, start // tile_cols + n))
    plan = (tuple(tiles), tuple(flips), tuple(windows), k_start, k_rows, base is not None, prev is not None, width, tile_cols)
    tile_rows = len(tiles) * TILE_ROWS
    vmem = vmem or 4 * n_layers * k_rows * (tile_rows + width) + 16 * TILE_ROWS * tile_cols + (8 << 20)
    return pl.pallas_call(
        functools.partial(product_kernel, plan),
        grid=(len(tiles), width // tile_cols),
        out_shape=out_shape,
        in_specs=in_specs,
        out_specs=out_spec,
        scratch_shapes=[
            pltpu.VMEM((2, tile_rows, n_layers * k_rows), jnp.bfloat16),
            pltpu.VMEM((2 * n_layers, k_rows, width), jnp.bfloat16),
            pltpu.SemaphoreType.DMA((2, len(tiles))),
            pltpu.SemaphoreType.DMA((2 * n_layers, width // tile_cols)),
        ],
        input_output_aliases=aliases,
        cost_estimate=pl.CostEstimate(flops=4 * tile_rows * n_layers * k_rows * width, bytes_accessed=4 * tile_rows * half, transcendentals=0),
        compiler_params=pltpu.CompilerParams(dimension_semantics=("arbitrary", "arbitrary"), vmem_limit_bytes=vmem),
        name="product",
    )(*operands)


def weight_kernel(layer_flip, *refs):
    a_own, a_far, out_ref, sems = refs[0], refs[1:-2], refs[-2], refs[-1]
    slice_rows = out_ref.shape[2]
    start = pl.multiple_of(lax.rem(lax.axis_index("depth") + layer_flip, 2) * slice_rows, slice_rows)
    copies = [pltpu.make_async_copy(a_own.at[:, pl.ds(start, slice_rows)], out_ref.at[0], sems.at[0])]
    for tile, ref in enumerate(a_far):
        block = out_ref.at[1, pl.ds(tile * TILE_ROWS, TILE_ROWS)]
        copies.append(pltpu.make_async_copy(ref.at[:, pl.ds(start, slice_rows)], block, sems.at[tile + 1]))
    for copy in copies:
        copy.start()
    for copy in copies:
        copy.wait()


def late_weights(a_own, a_far):
    rows, half = a_own.shape
    any_spec = pl.BlockSpec(memory_space=pl.ANY)
    return pl.pallas_call(
        functools.partial(weight_kernel, 1),
        out_shape=jax.ShapeDtypeStruct((2, rows, half // 2), jnp.bfloat16),
        in_specs=[any_spec] * (1 + len(a_far)),
        out_specs=pl.BlockSpec(memory_space=pltpu.VMEM),
        scratch_shapes=[pltpu.SemaphoreType.DMA((1 + len(a_far),))],
        cost_estimate=pl.CostEstimate(flops=2 * rows * half * 256, bytes_accessed=4 * rows * half, transcendentals=0),
        compiler_params=pltpu.CompilerParams(vmem_limit_bytes=16 << 20),
        name="late_weights",
    )(a_own, *a_far)


def late_kernel(k_start, base_start, target, *refs):
    weights, x_deep, x_both, base = refs[:4]
    rest = refs[4:]
    k_rows, width = x_deep.shape
    cross = lax.rem(lax.axis_index("col") + lax.axis_index("row"), 2)
    k_range = pl.ds(k_start, k_rows)

    def row_tile(tile, carry):
        row_range = pl.ds(pl.multiple_of(tile * TILE_ROWS, TILE_ROWS), TILE_ROWS)
        total = base[row_range, pl.ds(base_start, width)]
        total = total + jnp.dot(weights[cross, row_range, k_range], x_deep[...], preferred_element_type=jnp.float32)
        total = total + jnp.dot(weights[1 - cross, row_range, k_range], x_both[...], preferred_element_type=jnp.float32)
        if target is None:
            rest[0][row_range] = total
        else:
            y_ref, stage, sems = rest[1:]
            stage[row_range] = total.astype(stage.dtype)
            out_copy(tile, y_ref, stage, sems).start()
        return carry

    def out_copy(tile, y_ref, stage, sems):
        rhs_idx, start = target
        row_range = pl.ds(pl.multiple_of(tile * TILE_ROWS, TILE_ROWS), TILE_ROWS)
        return pltpu.make_async_copy(stage.at[row_range], y_ref.at[rhs_idx, row_range, pl.ds(start, width)], sems.at[tile])

    tiles = weights.shape[1] // TILE_ROWS
    lax.fori_loop(0, tiles, row_tile, 0)
    if target is not None:
        for tile in range(tiles):
            out_copy(tile, *rest[1:]).wait()


def late_product(weights, x_deep, x_both, base, base_start, k_start, prev=None, target=None):
    vmem_spec = pl.BlockSpec(memory_space=pltpu.VMEM)
    any_spec = pl.BlockSpec(memory_space=pl.ANY)
    rows, width = weights.shape[1], x_deep.shape[1]
    operands = [weights, x_deep, x_both, base]
    in_specs = [vmem_spec] * 4
    common = dict(
        name="late",
        compiler_params=pltpu.CompilerParams(vmem_limit_bytes=28 << 20),
        cost_estimate=pl.CostEstimate(flops=4 * rows * x_deep.size, bytes_accessed=4 * x_deep.size, transcendentals=0),
    )
    body = functools.partial(late_kernel, k_start, base_start, target)
    if target is None:
        return pl.pallas_call(body, out_shape=jax.ShapeDtypeStruct((rows, width), jnp.float32), in_specs=in_specs, out_specs=vmem_spec, **common)(*operands)
    return pl.pallas_call(
        body,
        out_shape=jax.ShapeDtypeStruct(prev.shape, prev.dtype),
        in_specs=in_specs + [any_spec],
        out_specs=any_spec,
        scratch_shapes=[pltpu.VMEM((rows, width), jnp.bfloat16), pltpu.SemaphoreType.DMA((rows // TILE_ROWS,))],
        input_output_aliases={4: 0},
        **common,
    )(*operands, prev)


OWN, DEEP, PEER, BOTH = (0, 0), (0, 1), (1, 0), (1, 1)


def solution(mesh):
    def permute(value, axis):
        return lax.ppermute(value, axis, SWAP)

    def body(w_local, x_local):
        y_shape = x_local.shape
        slice_rows = y_shape[1]
        n_row_tiles = w_local.shape[0] // TILE_ROWS

        def piece_of(x, chunk):
            rhs_idx, start, width, k_start, k_rows = chunk
            return x[rhs_idx, k_start : k_start + k_rows, start : start + width]

        sends = {SEND_ORDER[0]: piece_of(x_local, CHUNKS[SEND_ORDER[0]])}
        sends[SEND_ORDER[0]], x_rest = lax.optimization_barrier((sends[SEND_ORDER[0]], x_local))
        second = piece_of(x_rest, CHUNKS[SEND_ORDER[1]])
        sends[SEND_ORDER[1]], x_rest, w_rest = lax.optimization_barrier((second, x_rest, w_local))
        w_first, x_rest, w_rest = lax.optimization_barrier((w_rest[:TILE_ROWS], x_rest, w_rest))
        for idx in SEND_ORDER[2:]:
            sends[idx] = piece_of(x_rest, CHUNKS[idx])
        deep = {idx: permute(sends[idx], "depth") for idx in SEND_ORDER}
        w_sends = [w_first] + [w_rest[tile * TILE_ROWS : (tile + 1) * TILE_ROWS] for tile in range(1, n_row_tiles)]
        w_far = [permute(piece, "col") for piece in w_sends]
        x_row = permute(x_rest, "row")

        def full(idx, relay, y, tiles):
            rhs_idx, start, width, _, _ = CHUNKS[idx]
            window = (rhs_idx, start)
            return product(w_local, w_far, (x_local, deep[idx], x_row, relay), (OWN, DEEP, PEER, BOTH), (window, None, window, None), (0, slice_rows), width, tiles=tiles, prev=y, out=(y_shape, rhs_idx, start))

        def local(y, x_row, rhs_idx, start, width, tiles, prev=None):
            x_row, y = lax.optimization_barrier((x_row, y))
            window = (rhs_idx, start)
            base = product(w_local, w_far, (x_local, x_row), (OWN, PEER), (window, window), (0, slice_rows), width, tiles=tiles, prev=prev, vmem=LOCAL_VMEM)
            return lax.optimization_barrier((y, base))

        count = len(CHUNKS)
        late_rhs, late_start = CHUNKS[LATE][0], CHUNKS[LATE][1]
        main_width = sum(chunk[2] for chunk in CHUNKS[LATE : count - 3])

        relay_tail = permute(deep[count - 1], "row")
        relay0 = permute(deep[0], "row")
        y = full(0, relay0, None, (0,))
        y, base = local(y, x_row, late_rhs, late_start, main_width, (0,))
        y = full(0, relay0, y, (1,))
        piece, y = lax.optimization_barrier((deep[1], y))
        relay1 = permute(piece, "row")
        y = full(1, relay1, y, (0, 1))
        y, base = local(y, x_row, late_rhs, late_start, main_width, (1,), prev=base)
        y = full(0, relay0, y, (2,))
        y = full(1, relay1, y, (2,))
        for idx in range(2, count - 1):
            rhs_idx, start, _, k_start, _ = CHUNKS[idx]
            piece, y = lax.optimization_barrier((deep[idx], y))
            relay = permute(piece, "row")
            if idx < LATE:
                y = full(idx, relay, y, (0, 1, 2))
            else:
                part, offset = (base, start - late_start) if idx < count - 3 else (base_last, 0) if idx == count - 3 else (base_tail, 0)
                y = late_product(weights, piece, relay, part, offset, k_start, prev=y, target=(rhs_idx, start))
            if idx == LATE - 1:
                y, base = local(y, x_row, late_rhs, late_start, main_width, (2,), prev=base)
                w_gate, y = lax.optimization_barrier((w_local, y))
                weights = late_weights(w_gate, w_far)
                y, weights = lax.optimization_barrier((y, weights))
            if idx == LATE + 1:
                y, base_last = local(y, x_row, *CHUNKS[count - 3][:3], (0, 1, 2))
                y, base_tail = local(y, x_row, *CHUNKS[count - 1][:3], (0, 1, 2))
                piece, y = lax.optimization_barrier((deep[count - 1], y))
                base_tail = late_product(weights, piece, relay_tail, base_tail, 0, CHUNKS[count - 1][3])
                y, base_tail = lax.optimization_barrier((y, base_tail))
        return y

    return jax.shard_map(body, mesh=mesh, in_specs=(P(("row", "depth"), "col"), P(None, ("row", "depth"), "col")), out_specs=P(None, ("row", "depth"), "col"), check_vma=False)
```

```python
import functools

import jax
import jax.numpy as jnp
from jax import lax
from jax.experimental import pallas as pl
from jax.experimental.pallas import tpu as pltpu
from jax.sharding import PartitionSpec as P


SWAP = [(0, 1), (1, 0)]
CHUNKS = {
    "a": (0, 0, 512, 0, 1536),
    "b": (0, 512, 1536, 0, 1536),
    "c": (1, 0, 1024, 0, 1536),
    "d": (1, 1024, 1024, 0, 1536),
    "e": (2, 0, 512, 0, 1536),
    "f": (2, 512, 512, 0, 1536),
    "g": (2, 1024, 256, 0, 1536),
    "h": (2, 1280, 256, 0, 1536),
    "i0": (2, 1536, 256, 0, 768),
    "i1": (2, 1536, 256, 768, 768),
    "j0": (2, 1792, 256, 0, 384),
    "j1": (2, 1792, 256, 384, 640),
    "j2": (2, 1792, 256, 1024, 512),
}
SEND_ORDER = ("j0", "a", "b", "c", "d", "i0", "j1", "e", "f", "g", "h", "i1", "j2")
LATE_COLS = (2, 0, 2048)
TILE_ROWS = 512
TILE_COLS = 512
LOCAL_VMEM = 58 << 20
SMALL_ROWS = 1536


def product_kernel(plan, *refs):
    tiles, flips, windows, k_start, k_rows, has_base, has_prev, width, tile_cols = plan
    n_tiles, n_pieces = len(tiles), len(flips)
    a_own, a_far = refs[0], refs[1 : 1 + n_tiles]
    pieces = refs[1 + n_tiles : 1 + n_tiles + n_pieces]
    rest = refs[1 + n_tiles + n_pieces :]
    base_ref = rest[0] if has_base else None
    outs = rest[has_base + has_prev : -4]
    a_all, x_all, a_sems, x_sems = rest[-4:]
    slice_rows = a_own.shape[1] // 2
    layer_idx = lax.axis_index("depth")
    cross = lax.rem(lax.axis_index("col") + lax.axis_index("row"), 2)
    m, n = pl.program_id(0), pl.program_id(1)
    layers = sorted({flip_layer for _, flip_layer in flips})
    n_layers = len(layers)
    col_tiles = width // tile_cols

    def a_copy(side, tile):
        if side == 0:
            source = a_own.at[pl.ds(tiles[tile] * TILE_ROWS, TILE_ROWS)]
        else:
            source = a_far[tile]
        if n_layers == 1:
            start = lax.rem(layer_idx + layers[0], 2) * slice_rows + k_start
            source = source.at[:, pl.ds(pl.multiple_of(start, 128), k_rows)]
        return pltpu.make_async_copy(source, a_all.at[side, pl.ds(tile * TILE_ROWS, TILE_ROWS)], a_sems.at[side, tile])

    def x_copy(idx, tile):
        flip_row, flip_layer = flips[idx]
        slot = lax.rem(cross + flip_row, 2) * n_layers
        if n_layers == 2:
            slot = slot + lax.rem(layer_idx + flip_layer, 2)
        source = pieces[idx]
        start = tile * tile_cols
        if windows[idx] is not None:
            rhs_idx, offset = windows[idx]
            source = source.at[rhs_idx]
            start = start + offset
        return pltpu.make_async_copy(
            source.at[:, pl.ds(start, tile_cols)],
            x_all.at[slot, :, pl.ds(tile * tile_cols, tile_cols)],
            x_sems.at[slot, tile],
        )

    def x_wait(side, tile):
        for layer in range(n_layers):
            slot = side * n_layers + layer
            block = x_all.at[slot, :, pl.ds(tile * tile_cols, tile_cols)]
            pltpu.make_async_copy(block, block, x_sems.at[slot, tile]).wait()

    def x_start(side, tile):
        for idx, (flip_row, _) in enumerate(flips):
            @pl.when(lax.rem(cross + flip_row, 2) == side)
            def _():
                x_copy(idx, tile).start()

    groups = [(0, col, side) for col in range(col_tiles) for side in range(2)]
    groups += [(tile, 0, side) for tile in range(1, n_tiles) for side in range(2)]

    def group_start(index):
        if index < len(groups):
            tile, col, side = groups[index]
            if col == 0:
                a_copy(side, tile).start()
            if tile == 0:
                x_start(side, col)

    def group_wait(index):
        tile, col, side = groups[index]
        if col == 0:
            a_copy(side, tile).wait()
        if tile == 0:
            x_wait(side, col)

    row_range = pl.ds(pl.multiple_of(m * TILE_ROWS, TILE_ROWS), TILE_ROWS)
    col_range = pl.ds(pl.multiple_of(n * tile_cols, tile_cols), tile_cols)
    total = base_ref[...] if has_base else None
    for side in range(2):
        for index, (tile, col, group_side) in enumerate(groups):
            if group_side == side:
                @pl.when((m == tile) & (n == col))
                def _():
                    if index == 0:
                        group_start(0)
                    group_wait(index)
                    if index == 0:
                        group_start(1)
                    group_start(index + 2)

        x_side = x_all[pl.ds(side * n_layers, n_layers), :, col_range].reshape(n_layers * k_rows, tile_cols)
        term = jnp.dot(a_all[side, row_range], x_side, preferred_element_type=jnp.float32)
        total = term if total is None else total + term
    if len(outs[0].shape) == 3:
        outs[0][0] = total.astype(outs[0].dtype)
    else:
        for col, out_ref in enumerate(outs):
            @pl.when(n == col)
            def _():
                out_ref[...] = total


def product(a_own, a_far, pieces, flips, windows, k_range, width, tiles=(0, 1, 2), vmem=None, base=None, base_start=0, prev=None, out=None):
    rows, half = a_own.shape
    k_start, k_rows = k_range
    any_spec = pl.BlockSpec(memory_space=pl.ANY)
    tile_cols = min(TILE_COLS, width)
    n_layers = len({flip_layer for _, flip_layer in flips})
    operands = [a_own, *(a_far[tile] for tile in tiles), *pieces]
    hbm_spec = pl.BlockSpec(memory_space=pltpu.HBM)
    in_specs = [hbm_spec] * (1 + len(tiles)) + [any_spec if window is None else hbm_spec for window in windows]
    first = tiles[0]
    if base is not None:
        operands.append(base)
        in_specs.append(pl.BlockSpec((TILE_ROWS, tile_cols), lambda m, n: (first + m, base_start // tile_cols + n)))
    prevs = list(prev) if isinstance(prev, (list, tuple)) else [] if prev is None else [prev]
    aliases = {len(operands) + idx: idx for idx in range(len(prevs))}
    operands += prevs
    in_specs += [any_spec] * len(prevs)
    if out is None:
        out_shape = [jax.ShapeDtypeStruct((rows, tile_cols), jnp.float32)] * (width // tile_cols)
        out_spec = [pl.BlockSpec((TILE_ROWS, tile_cols), lambda m, n: (first + m, 0))] * len(out_shape)
    else:
        y_shape, rhs_idx, start = out
        out_shape = jax.ShapeDtypeStruct(y_shape, jnp.bfloat16)
        out_spec = pl.BlockSpec((1, TILE_ROWS, tile_cols), lambda m, n: (rhs_idx, first + m, start // tile_cols + n))
    plan = (tuple(tiles), tuple(flips), tuple(windows), k_start, k_rows, base is not None, len(prevs), width, tile_cols)
    tile_rows = len(tiles) * TILE_ROWS
    vmem = vmem or 4 * n_layers * k_rows * (tile_rows + width) + 16 * TILE_ROWS * tile_cols + (8 << 20)
    return pl.pallas_call(
        functools.partial(product_kernel, plan),
        grid=(len(tiles), width // tile_cols),
        out_shape=out_shape,
        in_specs=in_specs,
        out_specs=out_spec,
        scratch_shapes=[
            pltpu.VMEM((2, tile_rows, n_layers * k_rows), jnp.bfloat16),
            pltpu.VMEM((2 * n_layers, k_rows, width), jnp.bfloat16),
            pltpu.SemaphoreType.DMA((2, len(tiles))),
            pltpu.SemaphoreType.DMA((2 * n_layers, width // tile_cols)),
        ],
        input_output_aliases=aliases,
        cost_estimate=pl.CostEstimate(flops=4 * tile_rows * n_layers * k_rows * width, bytes_accessed=4 * tile_rows * half, transcendentals=0),
        compiler_params=pltpu.CompilerParams(dimension_semantics=("arbitrary", "arbitrary"), vmem_limit_bytes=vmem),
        name="product",
    )(*operands)


def weight_kernel(layer_flip, *refs):
    a_own, a_far, out_ref, sems = refs[0], refs[1:-2], refs[-2], refs[-1]
    slice_rows = out_ref.shape[2]
    start = pl.multiple_of(lax.rem(lax.axis_index("depth") + layer_flip, 2) * slice_rows, slice_rows)
    copies = [pltpu.make_async_copy(a_own.at[:, pl.ds(start, slice_rows)], out_ref.at[0], sems.at[0])]
    for tile, ref in enumerate(a_far):
        block = out_ref.at[1, pl.ds(tile * TILE_ROWS, TILE_ROWS)]
        copies.append(pltpu.make_async_copy(ref.at[:, pl.ds(start, slice_rows)], block, sems.at[tile + 1]))
    for copy in copies:
        copy.start()
    for copy in copies:
        copy.wait()


def late_weights(a_own, a_far):
    rows, half = a_own.shape
    any_spec = pl.BlockSpec(memory_space=pl.ANY)
    return pl.pallas_call(
        functools.partial(weight_kernel, 1),
        out_shape=jax.ShapeDtypeStruct((2, rows, half // 2), jnp.bfloat16),
        in_specs=[pl.BlockSpec(memory_space=pltpu.HBM)] * (1 + len(a_far)),
        out_specs=pl.BlockSpec(memory_space=pltpu.VMEM),
        scratch_shapes=[pltpu.SemaphoreType.DMA((1 + len(a_far),))],
        cost_estimate=pl.CostEstimate(flops=2 * rows * half * 256, bytes_accessed=4 * rows * half, transcendentals=0),
        compiler_params=pltpu.CompilerParams(vmem_limit_bytes=16 << 20),
        name="late_weights",
    )(a_own, *a_far)


def late_kernel(k_start, base_start, target, flips, tile_rows, *refs):
    n_pieces = len(flips)
    weights, pieces, base = refs[0], refs[1 : 1 + n_pieces], refs[1 + n_pieces]
    rest = refs[2 + n_pieces :]
    k_rows, width = pieces[0].shape
    cross = lax.rem(lax.axis_index("col") + lax.axis_index("row"), 2)
    k_range = pl.ds(k_start, k_rows)
    tiles = weights.shape[1] // tile_rows

    def rows_of(tile):
        return pl.ds(pl.multiple_of(tile * tile_rows, tile_rows), tile_rows)

    def out_copy(tile):
        y_ref, stage, sems = rest[1:]
        rhs_idx, start = target
        return pltpu.make_async_copy(stage.at[rows_of(tile)], y_ref.at[rhs_idx, rows_of(tile), pl.ds(start, width)], sems.at[tile])

    def row_tile(tile, carry):
        row_range = rows_of(tile)
        total = base[row_range, pl.ds(base_start, width)]
        for flip, piece in zip(flips, pieces):
            side = lax.rem(cross + flip, 2)
            total = total + jnp.dot(weights[side, row_range, k_range], piece[...], preferred_element_type=jnp.float32)
        if target is None:
            rest[0][row_range] = total
        else:
            stage = rest[2]
            stage[row_range] = total.astype(stage.dtype)
            out_copy(tile).start()
        return carry

    lax.fori_loop(0, tiles, row_tile, 0)
    if target is not None:
        for tile in range(tiles):
            out_copy(tile).wait()


def late_product(weights, pieces, flips, base, base_start, k_start, prev=None, target=None, tile_rows=TILE_ROWS):
    vmem_spec = pl.BlockSpec(memory_space=pltpu.VMEM)
    any_spec = pl.BlockSpec(memory_space=pl.ANY)
    rows, width = weights.shape[1], pieces[0].shape[1]
    operands = [weights, *pieces, base]
    in_specs = [vmem_spec] * len(operands)
    scratch = []
    aliases = {}
    if target is None:
        out_shape, out_spec = jax.ShapeDtypeStruct((rows, width), jnp.float32), vmem_spec
    else:
        out_shape, out_spec = jax.ShapeDtypeStruct(prev.shape, prev.dtype), any_spec
        aliases = {len(operands): 0}
        operands.append(prev)
        in_specs.append(any_spec)
        scratch = [pltpu.VMEM((rows, width), jnp.bfloat16), pltpu.SemaphoreType.DMA((rows // tile_rows,))]
    return pl.pallas_call(
        functools.partial(late_kernel, k_start, base_start, target, flips, tile_rows),
        out_shape=out_shape,
        in_specs=in_specs,
        out_specs=out_spec,
        scratch_shapes=scratch,
        input_output_aliases=aliases,
        name="late",
        compiler_params=pltpu.CompilerParams(vmem_limit_bytes=28 << 20),
        cost_estimate=pl.CostEstimate(flops=2 * rows * len(pieces) * pieces[0].size, bytes_accessed=4 * pieces[0].size, transcendentals=0),
    )(*operands)


OWN, DEEP, PEER, BOTH = (0, 0), (0, 1), (1, 0), (1, 1)


def solution(mesh):
    def permute(value, axis):
        return lax.ppermute(value, axis, SWAP)

    def body(w_local, x_local):
        y_shape = x_local.shape
        slice_rows = y_shape[1]
        n_row_tiles = w_local.shape[0] // TILE_ROWS

        def piece_of(x, chunk):
            rhs_idx, start, width, k_start, k_rows = chunk
            return x[rhs_idx, k_start : k_start + k_rows, start : start + width]

        sends = {SEND_ORDER[0]: piece_of(x_local, CHUNKS[SEND_ORDER[0]])}
        sends[SEND_ORDER[0]], x_rest = lax.optimization_barrier((sends[SEND_ORDER[0]], x_local))
        second = piece_of(x_rest, CHUNKS[SEND_ORDER[1]])
        sends[SEND_ORDER[1]], x_rest, w_rest = lax.optimization_barrier((second, x_rest, w_local))
        w_first, x_rest, w_rest = lax.optimization_barrier((w_rest[:TILE_ROWS], x_rest, w_rest))
        for name in SEND_ORDER[2:]:
            sends[name] = piece_of(x_rest, CHUNKS[name])
        deep = {name: permute(sends[name], "depth") for name in SEND_ORDER}
        w_sends = [w_first] + [w_rest[tile * TILE_ROWS : (tile + 1) * TILE_ROWS] for tile in range(1, n_row_tiles)]
        w_far = [permute(piece, "col") for piece in w_sends]
        x_row = permute(x_rest, "row")

        def full(name, relay, y, tiles):
            rhs_idx, start, width, _, _ = CHUNKS[name]
            window = (rhs_idx, start)
            return product(w_local, w_far, (x_local, deep[name], x_row, relay), (OWN, DEEP, PEER, BOTH), (window, None, window, None), (0, slice_rows), width, tiles=tiles, prev=y, out=(y_shape, rhs_idx, start))

        def local(y, tiles, prev=None):
            rhs_idx, start, width = LATE_COLS
            gated, y = lax.optimization_barrier((x_row, y))
            window = (rhs_idx, start)
            base = product(w_local, w_far, (x_local, gated), (OWN, PEER), (window, window), (0, slice_rows), width, tiles=tiles, prev=prev, vmem=LOCAL_VMEM)
            return lax.optimization_barrier((y, base))

        def relay_after(y, name):
            piece, y = lax.optimization_barrier((deep[name], y))
            return piece, permute(piece, "row"), y

        relay_j0 = permute(deep["j0"], "row")
        relay_a = permute(deep["a"], "row")
        y = full("a", relay_a, None, (0,))
        y, base = local(y, (0,))
        y = full("a", relay_a, y, (1,))
        _, relay, y = relay_after(y, "b")
        y = full("b", relay, y, (0, 1))
        y, base = local(y, (1,), prev=base)
        y = full("a", relay_a, y, (2,))
        y = full("b", relay, y, (2,))
        for name in ("c", "d"):
            _, relay, y = relay_after(y, name)
            y = full(name, relay, y, (0, 1, 2))
        early_i0, relay_i0, y = relay_after(y, "i0")
        early_j1, relay_j1, y = relay_after(y, "j1")
        y, base = local(y, (2,), prev=base)
        w_gate, y = lax.optimization_barrier((w_local, y))
        weights = late_weights(w_gate, w_far)
        y, weights = lax.optimization_barrier((y, weights))

        def base_of(name):
            _, start, _, _, _ = CHUNKS[name]
            return base[start // TILE_COLS], start % TILE_COLS

        def late(name, y):
            piece, relay, y = relay_after(y, name)
            rhs_idx, start, _, k_start, _ = CHUNKS[name]
            return late_product(weights, (piece, relay), (0, 1), *base_of(name), k_start, prev=y, target=(rhs_idx, start))

        def early_part(name, piece, relay, part, part_start):
            return late_product(weights, (piece, relay), (0, 1), part, part_start, CHUNKS[name][3])

        def split_late(name, y, part, part_start, tile_rows=TILE_ROWS):
            piece, relay, y = relay_after(y, name)
            rhs_idx, start, _, k_start, _ = CHUNKS[name]
            part = late_product(weights, (piece,), (0,), part, part_start, k_start, tile_rows=tile_rows)
            return late_product(weights, (relay,), (1,), part, 0, k_start, prev=y, target=(rhs_idx, start), tile_rows=tile_rows)

        part_j = early_part("j0", deep["j0"], relay_j0, *base_of("j0"))
        y, part_j = lax.optimization_barrier((y, part_j))
        y = late("e", y)
        part_i = early_part("i0", early_i0, relay_i0, *base_of("i0"))
        part_j = early_part("j1", early_j1, relay_j1, part_j, 0)
        y, part_i, part_j = lax.optimization_barrier((y, part_i, part_j))
        y = late("f", y)
        for name in ("g", "h"):
            y = split_late(name, y, *base_of(name))
        y = split_late("i1", y, part_i, 0, SMALL_ROWS)
        return split_late("j2", y, part_j, 0, SMALL_ROWS)

    return jax.shard_map(body, mesh=mesh, in_specs=(P(("row", "depth"), "col"), P(None, ("row", "depth"), "col")), out_specs=P(None, ("row", "depth"), "col"), check_vma=False)
```

```python
import functools

import jax
import jax.numpy as jnp
from jax import lax
from jax.experimental import pallas as pl
from jax.experimental.pallas import tpu as pltpu
from jax.sharding import PartitionSpec as P


SWAP = [(0, 1), (1, 0)]
CHUNKS = {
    "a": (0, 0, 512, 0, 1536),
    "b": (0, 512, 1536, 0, 1536),
    "c": (1, 0, 1024, 0, 1536),
    "d": (1, 1024, 1024, 0, 1536),
    "e": (2, 0, 512, 0, 1536),
    "f": (2, 512, 512, 0, 1536),
    "g": (2, 1024, 256, 0, 1536),
    "h": (2, 1280, 256, 0, 1536),
    "i0": (2, 1536, 256, 0, 1024),
    "i1": (2, 1536, 256, 1024, 512),
    "j0": (2, 1792, 256, 0, 384),
    "j1": (2, 1792, 256, 384, 768),
    "j2": (2, 1792, 256, 1152, 384),
}
SEND_ORDER = ("j0", "a", "b", "c", "d", "i0", "j1", "e", "f", "g", "h")
SENT_LATE = ("i1", "j2")
LATE_COLS = (2, 0, 2048)
TILE_ROWS = 512
TILE_COLS = 512
LOCAL_VMEM = 58 << 20
SMALL_ROWS = 1536


def product_kernel(plan, *refs):
    tiles, flips, windows, k_start, k_rows, has_base, has_prev, width, tile_cols = plan
    n_tiles, n_pieces = len(tiles), len(flips)
    a_own, a_far = refs[0], refs[1 : 1 + n_tiles]
    pieces = refs[1 + n_tiles : 1 + n_tiles + n_pieces]
    rest = refs[1 + n_tiles + n_pieces :]
    base_ref = rest[0] if has_base else None
    outs = rest[has_base + has_prev : -4]
    a_all, x_all, a_sems, x_sems = rest[-4:]
    slice_rows = a_own.shape[1] // 2
    layer_idx = lax.axis_index("depth")
    cross = lax.rem(lax.axis_index("col") + lax.axis_index("row"), 2)
    m, n = pl.program_id(0), pl.program_id(1)
    layers = sorted({flip_layer for _, flip_layer in flips})
    n_layers = len(layers)
    col_tiles = width // tile_cols

    def a_copy(side, tile):
        if side == 0:
            source = a_own.at[pl.ds(tiles[tile] * TILE_ROWS, TILE_ROWS)]
        else:
            source = a_far[tile]
        if n_layers == 1:
            start = lax.rem(layer_idx + layers[0], 2) * slice_rows + k_start
            source = source.at[:, pl.ds(pl.multiple_of(start, 128), k_rows)]
        return pltpu.make_async_copy(source, a_all.at[side, pl.ds(tile * TILE_ROWS, TILE_ROWS)], a_sems.at[side, tile])

    def x_copy(idx, tile):
        flip_row, flip_layer = flips[idx]
        slot = lax.rem(cross + flip_row, 2) * n_layers
        if n_layers == 2:
            slot = slot + lax.rem(layer_idx + flip_layer, 2)
        source = pieces[idx]
        start = tile * tile_cols
        if windows[idx] is not None:
            rhs_idx, offset = windows[idx]
            source = source.at[rhs_idx]
            start = start + offset
        return pltpu.make_async_copy(
            source.at[:, pl.ds(start, tile_cols)],
            x_all.at[slot, :, pl.ds(tile * tile_cols, tile_cols)],
            x_sems.at[slot, tile],
        )

    def x_wait(side, tile):
        for layer in range(n_layers):
            slot = side * n_layers + layer
            block = x_all.at[slot, :, pl.ds(tile * tile_cols, tile_cols)]
            pltpu.make_async_copy(block, block, x_sems.at[slot, tile]).wait()

    def x_start(side, tile):
        for idx, (flip_row, _) in enumerate(flips):
            @pl.when(lax.rem(cross + flip_row, 2) == side)
            def _():
                x_copy(idx, tile).start()

    groups = [(0, col, side) for col in range(col_tiles) for side in range(2)]
    groups += [(tile, 0, side) for tile in range(1, n_tiles) for side in range(2)]

    def group_start(index):
        if index < len(groups):
            tile, col, side = groups[index]
            if col == 0:
                a_copy(side, tile).start()
            if tile == 0:
                x_start(side, col)

    def group_wait(index):
        tile, col, side = groups[index]
        if col == 0:
            a_copy(side, tile).wait()
        if tile == 0:
            x_wait(side, col)

    row_range = pl.ds(pl.multiple_of(m * TILE_ROWS, TILE_ROWS), TILE_ROWS)
    col_range = pl.ds(pl.multiple_of(n * tile_cols, tile_cols), tile_cols)
    total = base_ref[...] if has_base else None
    for side in range(2):
        for index, (tile, col, group_side) in enumerate(groups):
            if group_side == side:
                @pl.when((m == tile) & (n == col))
                def _():
                    if index == 0:
                        group_start(0)
                    group_wait(index)
                    if index == 0:
                        group_start(1)
                    group_start(index + 2)

        x_side = x_all[pl.ds(side * n_layers, n_layers), :, col_range].reshape(n_layers * k_rows, tile_cols)
        term = jnp.dot(a_all[side, row_range], x_side, preferred_element_type=jnp.float32)
        total = term if total is None else total + term
    if len(outs[0].shape) == 3:
        outs[0][0] = total.astype(outs[0].dtype)
    else:
        for col, out_ref in enumerate(outs):
            @pl.when(n == col)
            def _():
                out_ref[...] = total


def product(a_own, a_far, pieces, flips, windows, k_range, width, tiles=(0, 1, 2), vmem=None, base=None, base_start=0, prev=None, out=None):
    rows, half = a_own.shape
    k_start, k_rows = k_range
    any_spec = pl.BlockSpec(memory_space=pl.ANY)
    tile_cols = min(TILE_COLS, width)
    n_layers = len({flip_layer for _, flip_layer in flips})
    operands = [a_own, *(a_far[tile] for tile in tiles), *pieces]
    hbm_spec = pl.BlockSpec(memory_space=pltpu.HBM)
    in_specs = [hbm_spec] * (1 + len(tiles)) + [any_spec if window is None else hbm_spec for window in windows]
    first = tiles[0]
    if base is not None:
        operands.append(base)
        in_specs.append(pl.BlockSpec((TILE_ROWS, tile_cols), lambda m, n: (first + m, base_start // tile_cols + n)))
    prevs = list(prev) if isinstance(prev, (list, tuple)) else [] if prev is None else [prev]
    aliases = {len(operands) + idx: idx for idx in range(len(prevs))}
    operands += prevs
    in_specs += [any_spec] * len(prevs)
    if out is None:
        out_shape = [jax.ShapeDtypeStruct((rows, tile_cols), jnp.float32)] * (width // tile_cols)
        out_spec = [pl.BlockSpec((TILE_ROWS, tile_cols), lambda m, n: (first + m, 0))] * len(out_shape)
    else:
        y_shape, rhs_idx, start = out
        out_shape = jax.ShapeDtypeStruct(y_shape, jnp.bfloat16)
        out_spec = pl.BlockSpec((1, TILE_ROWS, tile_cols), lambda m, n: (rhs_idx, first + m, start // tile_cols + n))
    plan = (tuple(tiles), tuple(flips), tuple(windows), k_start, k_rows, base is not None, len(prevs), width, tile_cols)
    tile_rows = len(tiles) * TILE_ROWS
    vmem = vmem or 4 * n_layers * k_rows * (tile_rows + width) + 16 * TILE_ROWS * tile_cols + (8 << 20)
    return pl.pallas_call(
        functools.partial(product_kernel, plan),
        grid=(len(tiles), width // tile_cols),
        out_shape=out_shape,
        in_specs=in_specs,
        out_specs=out_spec,
        scratch_shapes=[
            pltpu.VMEM((2, tile_rows, n_layers * k_rows), jnp.bfloat16),
            pltpu.VMEM((2 * n_layers, k_rows, width), jnp.bfloat16),
            pltpu.SemaphoreType.DMA((2, len(tiles))),
            pltpu.SemaphoreType.DMA((2 * n_layers, width // tile_cols)),
        ],
        input_output_aliases=aliases,
        cost_estimate=pl.CostEstimate(flops=4 * tile_rows * n_layers * k_rows * width, bytes_accessed=4 * tile_rows * half, transcendentals=0),
        compiler_params=pltpu.CompilerParams(dimension_semantics=("arbitrary", "arbitrary"), vmem_limit_bytes=vmem),
        name="product",
    )(*operands)


def weight_kernel(layer_flip, *refs):
    a_own, a_far, out_ref, sems = refs[0], refs[1:-2], refs[-2], refs[-1]
    slice_rows = out_ref.shape[2]
    start = pl.multiple_of(lax.rem(lax.axis_index("depth") + layer_flip, 2) * slice_rows, slice_rows)
    copies = [pltpu.make_async_copy(a_own.at[:, pl.ds(start, slice_rows)], out_ref.at[0], sems.at[0])]
    for tile, ref in enumerate(a_far):
        block = out_ref.at[1, pl.ds(tile * TILE_ROWS, TILE_ROWS)]
        copies.append(pltpu.make_async_copy(ref.at[:, pl.ds(start, slice_rows)], block, sems.at[tile + 1]))
    for copy in copies:
        copy.start()
    for copy in copies:
        copy.wait()


def late_weights(a_own, a_far):
    rows, half = a_own.shape
    any_spec = pl.BlockSpec(memory_space=pl.ANY)
    return pl.pallas_call(
        functools.partial(weight_kernel, 1),
        out_shape=jax.ShapeDtypeStruct((2, rows, half // 2), jnp.bfloat16),
        in_specs=[pl.BlockSpec(memory_space=pltpu.HBM)] * (1 + len(a_far)),
        out_specs=pl.BlockSpec(memory_space=pltpu.VMEM),
        scratch_shapes=[pltpu.SemaphoreType.DMA((1 + len(a_far),))],
        cost_estimate=pl.CostEstimate(flops=2 * rows * half * 256, bytes_accessed=4 * rows * half, transcendentals=0),
        compiler_params=pltpu.CompilerParams(vmem_limit_bytes=16 << 20),
        name="late_weights",
    )(a_own, *a_far)


def late_kernel(k_start, base_start, target, flips, tile_rows, *refs):
    n_pieces = len(flips)
    weights, pieces, base = refs[0], refs[1 : 1 + n_pieces], refs[1 + n_pieces]
    rest = refs[2 + n_pieces :]
    k_rows, width = pieces[0].shape
    cross = lax.rem(lax.axis_index("col") + lax.axis_index("row"), 2)
    k_range = pl.ds(k_start, k_rows)
    tiles = weights.shape[1] // tile_rows

    def rows_of(tile):
        return pl.ds(pl.multiple_of(tile * tile_rows, tile_rows), tile_rows)

    def out_copy(tile):
        y_ref, stage, sems = rest[1:]
        rhs_idx, start = target
        return pltpu.make_async_copy(stage.at[rows_of(tile)], y_ref.at[rhs_idx, rows_of(tile), pl.ds(start, width)], sems.at[tile])

    def row_tile(tile, carry):
        row_range = rows_of(tile)
        total = base[row_range, pl.ds(base_start, width)]
        for flip, piece in zip(flips, pieces):
            side = lax.rem(cross + flip, 2)
            total = total + jnp.dot(weights[side, row_range, k_range], piece[...], preferred_element_type=jnp.float32)
        if target is None:
            rest[0][row_range] = total
        else:
            stage = rest[2]
            stage[row_range] = total.astype(stage.dtype)
            out_copy(tile).start()
        return carry

    lax.fori_loop(0, tiles, row_tile, 0)
    if target is not None:
        for tile in range(tiles):
            out_copy(tile).wait()


def late_product(weights, pieces, flips, base, base_start, k_start, prev=None, target=None, tile_rows=TILE_ROWS):
    vmem_spec = pl.BlockSpec(memory_space=pltpu.VMEM)
    any_spec = pl.BlockSpec(memory_space=pl.ANY)
    rows, width = weights.shape[1], pieces[0].shape[1]
    operands = [weights, *pieces, base]
    in_specs = [vmem_spec] * len(operands)
    scratch = []
    aliases = {}
    if target is None:
        out_shape, out_spec = jax.ShapeDtypeStruct((rows, width), jnp.float32), vmem_spec
    else:
        out_shape, out_spec = jax.ShapeDtypeStruct(prev.shape, prev.dtype), any_spec
        aliases = {len(operands): 0}
        operands.append(prev)
        in_specs.append(any_spec)
        scratch = [pltpu.VMEM((rows, width), jnp.bfloat16), pltpu.SemaphoreType.DMA((rows // tile_rows,))]
    return pl.pallas_call(
        functools.partial(late_kernel, k_start, base_start, target, flips, tile_rows),
        out_shape=out_shape,
        in_specs=in_specs,
        out_specs=out_spec,
        scratch_shapes=scratch,
        input_output_aliases=aliases,
        name="late",
        compiler_params=pltpu.CompilerParams(vmem_limit_bytes=28 << 20),
        cost_estimate=pl.CostEstimate(flops=2 * rows * len(pieces) * pieces[0].size, bytes_accessed=4 * pieces[0].size, transcendentals=0),
    )(*operands)


OWN, DEEP, PEER, BOTH = (0, 0), (0, 1), (1, 0), (1, 1)


def solution(mesh):
    def permute(value, axis):
        return lax.ppermute(value, axis, SWAP)

    def body(w_local, x_local):
        y_shape = x_local.shape
        slice_rows = y_shape[1]
        n_row_tiles = w_local.shape[0] // TILE_ROWS

        def piece_of(x, chunk):
            rhs_idx, start, width, k_start, k_rows = chunk
            return x[rhs_idx, k_start : k_start + k_rows, start : start + width]

        sends = {SEND_ORDER[0]: piece_of(x_local, CHUNKS[SEND_ORDER[0]])}
        sends[SEND_ORDER[0]], x_rest = lax.optimization_barrier((sends[SEND_ORDER[0]], x_local))
        second = piece_of(x_rest, CHUNKS[SEND_ORDER[1]])
        sends[SEND_ORDER[1]], x_rest, w_rest = lax.optimization_barrier((second, x_rest, w_local))
        w_first, x_rest, w_rest = lax.optimization_barrier((w_rest[:TILE_ROWS], x_rest, w_rest))
        for name in SEND_ORDER[2:]:
            sends[name] = piece_of(x_rest, CHUNKS[name])
        deep = {name: permute(sends[name], "depth") for name in SEND_ORDER}
        w_sends = [w_first] + [w_rest[tile * TILE_ROWS : (tile + 1) * TILE_ROWS] for tile in range(1, n_row_tiles)]
        w_far = [permute(piece, "col") for piece in w_sends]
        x_row = permute(x_rest, "row")

        def full(name, relay, y, tiles):
            rhs_idx, start, width, _, _ = CHUNKS[name]
            window = (rhs_idx, start)
            return product(w_local, w_far, (x_local, deep[name], x_row, relay), (OWN, DEEP, PEER, BOTH), (window, None, window, None), (0, slice_rows), width, tiles=tiles, prev=y, out=(y_shape, rhs_idx, start))

        def local(y, tiles, prev=None):
            rhs_idx, start, width = LATE_COLS
            gated, y = lax.optimization_barrier((x_row, y))
            window = (rhs_idx, start)
            base = product(w_local, w_far, (x_local, gated), (OWN, PEER), (window, window), (0, slice_rows), width, tiles=tiles, prev=prev, vmem=LOCAL_VMEM)
            return lax.optimization_barrier((y, base))

        def relay_after(y, name):
            piece, y = lax.optimization_barrier((deep[name], y))
            return piece, permute(piece, "row"), y

        relay_j0 = permute(deep["j0"], "row")
        relay_a = permute(deep["a"], "row")
        y = full("a", relay_a, None, (0,))
        y, base = local(y, (0,))
        y = full("a", relay_a, y, (1,))
        _, relay, y = relay_after(y, "b")
        y = full("b", relay, y, (0, 1))
        y, base = local(y, (1,), prev=base)
        y = full("a", relay_a, y, (2,))
        y = full("b", relay, y, (2,))
        for name in ("c", "d"):
            _, relay, y = relay_after(y, name)
            y = full(name, relay, y, (0, 1, 2))
        early_i0, relay_i0, y = relay_after(y, "i0")
        early_j1, relay_j1, y = relay_after(y, "j1")
        y, base = local(y, (2,), prev=base)
        w_gate, y = lax.optimization_barrier((w_local, y))
        weights = late_weights(w_gate, w_far)
        y, weights = lax.optimization_barrier((y, weights))

        def base_of(name):
            _, start, _, _, _ = CHUNKS[name]
            return base[start // TILE_COLS], start % TILE_COLS

        def late(name, y):
            piece, relay, y = relay_after(y, name)
            rhs_idx, start, _, k_start, _ = CHUNKS[name]
            return late_product(weights, (piece, relay), (0, 1), *base_of(name), k_start, prev=y, target=(rhs_idx, start))

        def early_part(name, piece, relay, part, part_start):
            return late_product(weights, (piece, relay), (0, 1), part, part_start, CHUNKS[name][3])

        def split_late(name, y, part, part_start, tile_rows=TILE_ROWS):
            piece, relay, y = relay_after(y, name)
            rhs_idx, start, _, k_start, _ = CHUNKS[name]
            part = late_product(weights, (piece,), (0,), part, part_start, k_start, tile_rows=tile_rows)
            return late_product(weights, (relay,), (1,), part, 0, k_start, prev=y, target=(rhs_idx, start), tile_rows=tile_rows)

        part_j = early_part("j0", deep["j0"], relay_j0, *base_of("j0"))
        y, part_j = lax.optimization_barrier((y, part_j))
        y = late("e", y)
        part_i = early_part("i0", early_i0, relay_i0, *base_of("i0"))
        part_j = early_part("j1", early_j1, relay_j1, part_j, 0)
        y, part_i, part_j = lax.optimization_barrier((y, part_i, part_j))
        y = late("f", y)
        x_gate, y = lax.optimization_barrier((x_local, y))
        for name in SENT_LATE:
            deep[name] = permute(piece_of(x_gate, CHUNKS[name]), "depth")
        for name in ("g", "h"):
            y = split_late(name, y, *base_of(name))
        y = split_late("i1", y, part_i, 0, SMALL_ROWS)
        return split_late("j2", y, part_j, 0, SMALL_ROWS)

    return jax.shard_map(body, mesh=mesh, in_specs=(P(("row", "depth"), "col"), P(None, ("row", "depth"), "col")), out_specs=P(None, ("row", "depth"), "col"), check_vma=False)
```

```python
import functools

import jax
import jax.numpy as jnp
from jax import lax
from jax.experimental import pallas as pl
from jax.experimental.pallas import tpu as pltpu
from jax.sharding import PartitionSpec as P


SWAP = [(0, 1), (1, 0)]
CHUNKS = {
    "a": (0, 0, 512, 0, 1536),
    "b": (0, 512, 1536, 0, 1536),
    "c": (1, 0, 1024, 0, 1536),
    "d": (1, 1024, 1024, 0, 1536),
    "e": (2, 0, 512, 0, 1536),
    "f": (2, 512, 512, 0, 1536),
    "g": (2, 1024, 256, 0, 1536),
    "h": (2, 1280, 256, 0, 1536),
    "i0": (2, 1536, 256, 0, 1024),
    "i1": (2, 1536, 256, 1024, 512),
    "j0": (2, 1792, 256, 0, 384),
    "j1": (2, 1792, 256, 384, 768),
    "j2": (2, 1792, 256, 1152, 384),
}
SEND_ORDER = ("j0", "a", "b", "c", "d", "i0", "j1", "e", "f", "g", "h")
SENT_LATE = ("i1", "j2")
LATE_COLS = (2, 0, 2048)
TILE_ROWS = 512
TILE_COLS = 512
LOCAL_VMEM = 58 << 20
SMALL_ROWS = 1536


def product_kernel(plan, *refs):
    tiles, flips, windows, k_start, k_rows, has_base, has_prev, width, tile_cols = plan
    n_tiles, n_pieces = len(tiles), len(flips)
    a_own, a_far = refs[0], refs[1 : 1 + n_tiles]
    pieces = refs[1 + n_tiles : 1 + n_tiles + n_pieces]
    rest = refs[1 + n_tiles + n_pieces :]
    base_ref = rest[0] if has_base else None
    outs = rest[has_base + has_prev : -4]
    a_all, x_all, a_sems, x_sems = rest[-4:]
    slice_rows = a_own.shape[1] // 2
    layer_idx = lax.axis_index("depth")
    cross = lax.rem(lax.axis_index("col") + lax.axis_index("row"), 2)
    m, n = pl.program_id(0), pl.program_id(1)
    layers = sorted({flip_layer for _, flip_layer in flips})
    n_layers = len(layers)
    col_tiles = width // tile_cols

    def a_copy(side, tile):
        if side == 0:
            source = a_own.at[pl.ds(tiles[tile] * TILE_ROWS, TILE_ROWS)]
        else:
            source = a_far[tile]
        if n_layers == 1:
            start = lax.rem(layer_idx + layers[0], 2) * slice_rows + k_start
            source = source.at[:, pl.ds(pl.multiple_of(start, 128), k_rows)]
        return pltpu.make_async_copy(source, a_all.at[side, pl.ds(tile * TILE_ROWS, TILE_ROWS)], a_sems.at[side, tile])

    def x_copy(idx, tile):
        flip_row, flip_layer = flips[idx]
        slot = lax.rem(cross + flip_row, 2) * n_layers
        if n_layers == 2:
            slot = slot + lax.rem(layer_idx + flip_layer, 2)
        source = pieces[idx]
        start = tile * tile_cols
        if windows[idx] is not None:
            rhs_idx, offset = windows[idx]
            source = source.at[rhs_idx]
            start = start + offset
        return pltpu.make_async_copy(
            source.at[:, pl.ds(start, tile_cols)],
            x_all.at[slot, :, pl.ds(tile * tile_cols, tile_cols)],
            x_sems.at[slot, tile],
        )

    def x_wait(side, tile):
        for layer in range(n_layers):
            slot = side * n_layers + layer
            block = x_all.at[slot, :, pl.ds(tile * tile_cols, tile_cols)]
            pltpu.make_async_copy(block, block, x_sems.at[slot, tile]).wait()

    def x_start(side, tile):
        for idx, (flip_row, _) in enumerate(flips):
            @pl.when(lax.rem(cross + flip_row, 2) == side)
            def _():
                x_copy(idx, tile).start()

    groups = [(0, col, side) for col in range(col_tiles) for side in range(2)]
    groups += [(tile, 0, side) for tile in range(1, n_tiles) for side in range(2)]

    ahead = len(groups)

    def group_start(index):
        if index < len(groups):
            tile, col, side = groups[index]
            if col == 0:
                a_copy(side, tile).start()
            if tile == 0:
                x_start(side, col)

    def group_wait(index):
        tile, col, side = groups[index]
        if col == 0:
            a_copy(side, tile).wait()
        if tile == 0:
            x_wait(side, col)

    row_range = pl.ds(pl.multiple_of(m * TILE_ROWS, TILE_ROWS), TILE_ROWS)
    col_range = pl.ds(pl.multiple_of(n * tile_cols, tile_cols), tile_cols)
    total = base_ref[...] if has_base else None
    for side in range(2):
        for index, (tile, col, group_side) in enumerate(groups):
            if group_side == side:
                @pl.when((m == tile) & (n == col))
                def _():
                    if index == 0:
                        group_start(0)
                    group_wait(index)
                    for later in range(index + ahead if index else 1, index + ahead + 1):
                        group_start(later)

        x_side = x_all[pl.ds(side * n_layers, n_layers), :, col_range].reshape(n_layers * k_rows, tile_cols)
        term = jnp.dot(a_all[side, row_range], x_side, preferred_element_type=jnp.float32)
        total = term if total is None else total + term
    if len(outs[0].shape) == 3:
        outs[0][0] = total.astype(outs[0].dtype)
    else:
        for col, out_ref in enumerate(outs):
            @pl.when(n == col)
            def _():
                out_ref[...] = total


def product(a_own, a_far, pieces, flips, windows, k_range, width, tiles=(0, 1, 2), vmem=None, base=None, base_start=0, prev=None, out=None):
    rows, half = a_own.shape
    k_start, k_rows = k_range
    any_spec = pl.BlockSpec(memory_space=pl.ANY)
    tile_cols = min(TILE_COLS, width)
    n_layers = len({flip_layer for _, flip_layer in flips})
    operands = [a_own, *(a_far[tile] for tile in tiles), *pieces]
    hbm_spec = pl.BlockSpec(memory_space=pltpu.HBM)
    in_specs = [hbm_spec] * (1 + len(tiles)) + [any_spec if window is None else hbm_spec for window in windows]
    first = tiles[0]
    if base is not None:
        operands.append(base)
        in_specs.append(pl.BlockSpec((TILE_ROWS, tile_cols), lambda m, n: (first + m, base_start // tile_cols + n)))
    prevs = list(prev) if isinstance(prev, (list, tuple)) else [] if prev is None else [prev]
    aliases = {len(operands) + idx: idx for idx in range(len(prevs))}
    operands += prevs
    in_specs += [any_spec] * len(prevs)
    if out is None:
        out_shape = [jax.ShapeDtypeStruct((rows, tile_cols), jnp.float32)] * (width // tile_cols)
        out_spec = [pl.BlockSpec((TILE_ROWS, tile_cols), lambda m, n: (first + m, 0))] * len(out_shape)
    else:
        y_shape, rhs_idx, start = out
        out_shape = jax.ShapeDtypeStruct(y_shape, jnp.bfloat16)
        out_spec = pl.BlockSpec((1, TILE_ROWS, tile_cols), lambda m, n: (rhs_idx, first + m, start // tile_cols + n))
    plan = (tuple(tiles), tuple(flips), tuple(windows), k_start, k_rows, base is not None, len(prevs), width, tile_cols)
    tile_rows = len(tiles) * TILE_ROWS
    vmem = vmem or 4 * n_layers * k_rows * (tile_rows + width) + 16 * TILE_ROWS * tile_cols + (8 << 20)
    return pl.pallas_call(
        functools.partial(product_kernel, plan),
        grid=(len(tiles), width // tile_cols),
        out_shape=out_shape,
        in_specs=in_specs,
        out_specs=out_spec,
        scratch_shapes=[
            pltpu.VMEM((2, tile_rows, n_layers * k_rows), jnp.bfloat16),
            pltpu.VMEM((2 * n_layers, k_rows, width), jnp.bfloat16),
            pltpu.SemaphoreType.DMA((2, len(tiles))),
            pltpu.SemaphoreType.DMA((2 * n_layers, width // tile_cols)),
        ],
        input_output_aliases=aliases,
        cost_estimate=pl.CostEstimate(flops=4 * tile_rows * n_layers * k_rows * width, bytes_accessed=4 * tile_rows * half, transcendentals=0),
        compiler_params=pltpu.CompilerParams(dimension_semantics=("arbitrary", "arbitrary"), vmem_limit_bytes=vmem),
        name="product",
    )(*operands)


def weight_kernel(layer_flip, *refs):
    a_own, a_far, out_ref, sems = refs[0], refs[1:-2], refs[-2], refs[-1]
    slice_rows = out_ref.shape[2]
    start = pl.multiple_of(lax.rem(lax.axis_index("depth") + layer_flip, 2) * slice_rows, slice_rows)
    copies = [pltpu.make_async_copy(a_own.at[:, pl.ds(start, slice_rows)], out_ref.at[0], sems.at[0])]
    for tile, ref in enumerate(a_far):
        block = out_ref.at[1, pl.ds(tile * TILE_ROWS, TILE_ROWS)]
        copies.append(pltpu.make_async_copy(ref.at[:, pl.ds(start, slice_rows)], block, sems.at[tile + 1]))
    for copy in copies:
        copy.start()
    for copy in copies:
        copy.wait()


def late_weights(a_own, a_far):
    rows, half = a_own.shape
    any_spec = pl.BlockSpec(memory_space=pl.ANY)
    return pl.pallas_call(
        functools.partial(weight_kernel, 1),
        out_shape=jax.ShapeDtypeStruct((2, rows, half // 2), jnp.bfloat16),
        in_specs=[pl.BlockSpec(memory_space=pltpu.HBM)] * (1 + len(a_far)),
        out_specs=pl.BlockSpec(memory_space=pltpu.VMEM),
        scratch_shapes=[pltpu.SemaphoreType.DMA((1 + len(a_far),))],
        cost_estimate=pl.CostEstimate(flops=2 * rows * half * 256, bytes_accessed=4 * rows * half, transcendentals=0),
        compiler_params=pltpu.CompilerParams(vmem_limit_bytes=16 << 20),
        name="late_weights",
    )(a_own, *a_far)


def late_kernel(k_start, base_start, target, flips, tile_rows, *refs):
    n_pieces = len(flips)
    weights, pieces, base = refs[0], refs[1 : 1 + n_pieces], refs[1 + n_pieces]
    rest = refs[2 + n_pieces :]
    k_rows, width = pieces[0].shape
    cross = lax.rem(lax.axis_index("col") + lax.axis_index("row"), 2)
    k_range = pl.ds(k_start, k_rows)
    tiles = weights.shape[1] // tile_rows

    def rows_of(tile):
        return pl.ds(pl.multiple_of(tile * tile_rows, tile_rows), tile_rows)

    def out_copy(tile):
        y_ref, stage, sems = rest[1:]
        rhs_idx, start = target
        return pltpu.make_async_copy(stage.at[rows_of(tile)], y_ref.at[rhs_idx, rows_of(tile), pl.ds(start, width)], sems.at[tile])

    def row_tile(tile, carry):
        row_range = rows_of(tile)
        total = base[row_range, pl.ds(base_start, width)]
        for flip, piece in zip(flips, pieces):
            side = lax.rem(cross + flip, 2)
            total = total + jnp.dot(weights[side, row_range, k_range], piece[...], preferred_element_type=jnp.float32)
        if target is None:
            rest[0][row_range] = total
        else:
            stage = rest[2]
            stage[row_range] = total.astype(stage.dtype)
            out_copy(tile).start()
        return carry

    lax.fori_loop(0, tiles, row_tile, 0)
    if target is not None:
        for tile in range(tiles):
            out_copy(tile).wait()


def late_product(weights, pieces, flips, base, base_start, k_start, prev=None, target=None, tile_rows=TILE_ROWS):
    vmem_spec = pl.BlockSpec(memory_space=pltpu.VMEM)
    any_spec = pl.BlockSpec(memory_space=pl.ANY)
    rows, width = weights.shape[1], pieces[0].shape[1]
    operands = [weights, *pieces, base]
    in_specs = [vmem_spec] * len(operands)
    scratch = []
    aliases = {}
    if target is None:
        out_shape, out_spec = jax.ShapeDtypeStruct((rows, width), jnp.float32), vmem_spec
    else:
        out_shape, out_spec = jax.ShapeDtypeStruct(prev.shape, prev.dtype), any_spec
        aliases = {len(operands): 0}
        operands.append(prev)
        in_specs.append(any_spec)
        scratch = [pltpu.VMEM((rows, width), jnp.bfloat16), pltpu.SemaphoreType.DMA((rows // tile_rows,))]
    return pl.pallas_call(
        functools.partial(late_kernel, k_start, base_start, target, flips, tile_rows),
        out_shape=out_shape,
        in_specs=in_specs,
        out_specs=out_spec,
        scratch_shapes=scratch,
        input_output_aliases=aliases,
        name="late",
        compiler_params=pltpu.CompilerParams(vmem_limit_bytes=28 << 20),
        cost_estimate=pl.CostEstimate(flops=2 * rows * len(pieces) * pieces[0].size, bytes_accessed=4 * pieces[0].size, transcendentals=0),
    )(*operands)


OWN, DEEP, PEER, BOTH = (0, 0), (0, 1), (1, 0), (1, 1)


def solution(mesh):
    def permute(value, axis):
        return lax.ppermute(value, axis, SWAP)

    def body(w_local, x_local):
        y_shape = x_local.shape
        slice_rows = y_shape[1]
        n_row_tiles = w_local.shape[0] // TILE_ROWS

        def piece_of(x, chunk):
            rhs_idx, start, width, k_start, k_rows = chunk
            return x[rhs_idx, k_start : k_start + k_rows, start : start + width]

        sends = {SEND_ORDER[0]: piece_of(x_local, CHUNKS[SEND_ORDER[0]])}
        sends[SEND_ORDER[0]], x_rest = lax.optimization_barrier((sends[SEND_ORDER[0]], x_local))
        second = piece_of(x_rest, CHUNKS[SEND_ORDER[1]])
        sends[SEND_ORDER[1]], x_rest, w_rest = lax.optimization_barrier((second, x_rest, w_local))
        w_first, x_rest, w_rest = lax.optimization_barrier((w_rest[:TILE_ROWS], x_rest, w_rest))
        for name in SEND_ORDER[2:]:
            sends[name] = piece_of(x_rest, CHUNKS[name])
        deep = {name: permute(sends[name], "depth") for name in SEND_ORDER}
        w_sends = [w_first] + [w_rest[tile * TILE_ROWS : (tile + 1) * TILE_ROWS] for tile in range(1, n_row_tiles)]
        w_far = [permute(piece, "col") for piece in w_sends]
        x_row = permute(x_rest, "row")

        def full(name, relay, y, tiles):
            rhs_idx, start, width, _, _ = CHUNKS[name]
            window = (rhs_idx, start)
            return product(w_local, w_far, (x_local, deep[name], x_row, relay), (OWN, DEEP, PEER, BOTH), (window, None, window, None), (0, slice_rows), width, tiles=tiles, prev=y, out=(y_shape, rhs_idx, start))

        def local(y, tiles, prev=None):
            rhs_idx, start, width = LATE_COLS
            gated, y = lax.optimization_barrier((x_row, y))
            window = (rhs_idx, start)
            base = product(w_local, w_far, (x_local, gated), (OWN, PEER), (window, window), (0, slice_rows), width, tiles=tiles, prev=prev, vmem=LOCAL_VMEM)
            return lax.optimization_barrier((y, base))

        def relay_after(y, name):
            piece, y = lax.optimization_barrier((deep[name], y))
            return piece, permute(piece, "row"), y

        relay_j0 = permute(deep["j0"], "row")
        relay_a = permute(deep["a"], "row")
        y = full("a", relay_a, None, (0,))
        y, base = local(y, (0,))
        y = full("a", relay_a, y, (1,))
        _, relay, y = relay_after(y, "b")
        y = full("b", relay, y, (0, 1))
        y, base = local(y, (1,), prev=base)
        y = full("a", relay_a, y, (2,))
        y = full("b", relay, y, (2,))
        for name in ("c", "d"):
            _, relay, y = relay_after(y, name)
            y = full(name, relay, y, (0, 1, 2))
        early_i0, relay_i0, y = relay_after(y, "i0")
        early_j1, relay_j1, y = relay_after(y, "j1")
        y, base = local(y, (2,), prev=base)
        w_gate, y = lax.optimization_barrier((w_local, y))
        weights = late_weights(w_gate, w_far)
        y, weights = lax.optimization_barrier((y, weights))

        def base_of(name):
            _, start, _, _, _ = CHUNKS[name]
            return base[start // TILE_COLS], start % TILE_COLS

        def late(name, y):
            piece, relay, y = relay_after(y, name)
            rhs_idx, start, _, k_start, _ = CHUNKS[name]
            return late_product(weights, (piece, relay), (0, 1), *base_of(name), k_start, prev=y, target=(rhs_idx, start))

        def early_part(name, piece, relay, part, part_start):
            return late_product(weights, (piece, relay), (0, 1), part, part_start, CHUNKS[name][3])

        def split_late(name, y, part, part_start, tile_rows=TILE_ROWS):
            piece, relay, y = relay_after(y, name)
            rhs_idx, start, _, k_start, _ = CHUNKS[name]
            part = late_product(weights, (piece,), (0,), part, part_start, k_start, tile_rows=tile_rows)
            return late_product(weights, (relay,), (1,), part, 0, k_start, prev=y, target=(rhs_idx, start), tile_rows=tile_rows)

        part_j = early_part("j0", deep["j0"], relay_j0, *base_of("j0"))
        y, part_j = lax.optimization_barrier((y, part_j))
        y = late("e", y)
        part_i = early_part("i0", early_i0, relay_i0, *base_of("i0"))
        part_j = early_part("j1", early_j1, relay_j1, part_j, 0)
        y, part_i, part_j = lax.optimization_barrier((y, part_i, part_j))
        y = late("f", y)
        x_gate, y = lax.optimization_barrier((x_local, y))
        for name in SENT_LATE:
            deep[name] = permute(piece_of(x_gate, CHUNKS[name]), "depth")
        for name in ("g", "h"):
            y = split_late(name, y, *base_of(name))
        y = split_late("i1", y, part_i, 0, SMALL_ROWS)
        return split_late("j2", y, part_j, 0, SMALL_ROWS)

    return jax.shard_map(body, mesh=mesh, in_specs=(P(("row", "depth"), "col"), P(None, ("row", "depth"), "col")), out_specs=P(None, ("row", "depth"), "col"), check_vma=False)
```

```python
import functools

import jax
import jax.numpy as jnp
from jax import lax
from jax.experimental import pallas as pl
from jax.experimental.pallas import tpu as pltpu
from jax.sharding import PartitionSpec as P


SWAP = [(0, 1), (1, 0)]
CHUNKS = {
    "a": (0, 0, 512, 0, 1536),
    "b": (0, 512, 1536, 0, 1536),
    "c": (1, 0, 1024, 0, 1536),
    "d": (1, 1024, 1024, 0, 1536),
    "e": (2, 0, 512, 0, 1536),
    "f": (2, 512, 512, 0, 1536),
    "g": (2, 1024, 256, 0, 1536),
    "h": (2, 1280, 256, 0, 1536),
    "i0": (2, 1536, 256, 0, 1024),
    "i1": (2, 1536, 256, 1024, 512),
    "j0": (2, 1792, 256, 0, 384),
    "j1": (2, 1792, 256, 384, 768),
    "j2": (2, 1792, 256, 1152, 384),
}
SEND_ORDER = ("j0", "a", "b", "c", "d", "i0", "j1", "e", "f", "g", "h")
SENT_LATE = ("i1", "j2")
LATE_COLS = (2, 0, 2048)
TILE_ROWS = 512
TILE_COLS = 512
LOCAL_VMEM = 58 << 20
SMALL_ROWS = 1536


def product_kernel(plan, *refs):
    tiles, flips, windows, k_start, k_rows, has_base, has_prev, width, tile_cols = plan
    n_tiles, n_pieces = len(tiles), len(flips)
    a_own, a_far = refs[0], refs[1 : 1 + n_tiles]
    pieces = refs[1 + n_tiles : 1 + n_tiles + n_pieces]
    rest = refs[1 + n_tiles + n_pieces :]
    base_ref = rest[0] if has_base else None
    outs = rest[has_base + has_prev : -4]
    a_all, x_all, a_sems, x_sems = rest[-4:]
    slice_rows = a_own.shape[1] // 2
    layer_idx = lax.axis_index("depth")
    cross = lax.rem(lax.axis_index("col") + lax.axis_index("row"), 2)
    m, n = pl.program_id(0), pl.program_id(1)
    layers = sorted({flip_layer for _, flip_layer in flips})
    n_layers = len(layers)
    col_tiles = width // tile_cols

    def a_copy(side, tile):
        if side == 0:
            source = a_own.at[pl.ds(tiles[tile] * TILE_ROWS, TILE_ROWS)]
        else:
            source = a_far[tile]
        if n_layers == 1:
            start = lax.rem(layer_idx + layers[0], 2) * slice_rows + k_start
            source = source.at[:, pl.ds(pl.multiple_of(start, 128), k_rows)]
        return pltpu.make_async_copy(source, a_all.at[side, pl.ds(tile * TILE_ROWS, TILE_ROWS)], a_sems.at[side, tile])

    def x_copy(idx, tile):
        flip_row, flip_layer = flips[idx]
        slot = lax.rem(cross + flip_row, 2) * n_layers
        if n_layers == 2:
            slot = slot + lax.rem(layer_idx + flip_layer, 2)
        source = pieces[idx]
        start = tile * tile_cols
        if windows[idx] is not None:
            rhs_idx, offset = windows[idx]
            source = source.at[rhs_idx]
            start = start + offset
        return pltpu.make_async_copy(
            source.at[:, pl.ds(start, tile_cols)],
            x_all.at[slot, :, pl.ds(tile * tile_cols, tile_cols)],
            x_sems.at[slot, tile],
        )

    def x_wait(side, tile):
        for layer in range(n_layers):
            slot = side * n_layers + layer
            block = x_all.at[slot, :, pl.ds(tile * tile_cols, tile_cols)]
            pltpu.make_async_copy(block, block, x_sems.at[slot, tile]).wait()

    def x_start(side, tile):
        for idx, (flip_row, _) in enumerate(flips):
            @pl.when(lax.rem(cross + flip_row, 2) == side)
            def _():
                x_copy(idx, tile).start()

    groups = [(0, col, side) for col in range(col_tiles) for side in range(2)]
    groups += [(tile, 0, side) for tile in range(1, n_tiles) for side in range(2)]

    def group_start(index):
        if index < len(groups):
            tile, col, side = groups[index]
            if col == 0:
                a_copy(side, tile).start()
            if tile == 0:
                x_start(side, col)

    def group_wait(index):
        tile, col, side = groups[index]
        if col == 0:
            a_copy(side, tile).wait()
        if tile == 0:
            x_wait(side, col)

    row_range = pl.ds(pl.multiple_of(m * TILE_ROWS, TILE_ROWS), TILE_ROWS)
    col_range = pl.ds(pl.multiple_of(n * tile_cols, tile_cols), tile_cols)
    total = base_ref[...] if has_base else None
    for side in range(2):
        for index, (tile, col, group_side) in enumerate(groups):
            if group_side == side:
                @pl.when((m == tile) & (n == col))
                def _():
                    if index == 0:
                        group_start(0)
                    group_wait(index)
                    if index == 0:
                        group_start(1)
                    group_start(index + 2)

        x_side = x_all[pl.ds(side * n_layers, n_layers), :, col_range].reshape(n_layers * k_rows, tile_cols)
        term = jnp.dot(a_all[side, row_range], x_side, preferred_element_type=jnp.float32)
        total = term if total is None else total + term
    if len(outs[0].shape) == 3:
        outs[0][0] = total.astype(outs[0].dtype)
    else:
        for col, out_ref in enumerate(outs):
            @pl.when(n == col)
            def _():
                out_ref[...] = total


def product(a_own, a_far, pieces, flips, windows, k_range, width, tiles=(0, 1, 2), vmem=None, base=None, base_start=0, prev=None, out=None):
    rows, half = a_own.shape
    k_start, k_rows = k_range
    any_spec = pl.BlockSpec(memory_space=pl.ANY)
    tile_cols = min(TILE_COLS, width)
    n_layers = len({flip_layer for _, flip_layer in flips})
    operands = [a_own, *(a_far[tile] for tile in tiles), *pieces]
    hbm_spec = pl.BlockSpec(memory_space=pltpu.HBM)
    in_specs = [hbm_spec] * (1 + len(tiles)) + [any_spec if window is None else hbm_spec for window in windows]
    first = tiles[0]
    if base is not None:
        operands.append(base)
        in_specs.append(pl.BlockSpec((TILE_ROWS, tile_cols), lambda m, n: (first + m, base_start // tile_cols + n)))
    prevs = list(prev) if isinstance(prev, (list, tuple)) else [] if prev is None else [prev]
    aliases = {len(operands) + idx: idx for idx in range(len(prevs))}
    operands += prevs
    in_specs += [any_spec] * len(prevs)
    if out is None:
        out_shape = [jax.ShapeDtypeStruct((rows, tile_cols), jnp.float32)] * (width // tile_cols)
        out_spec = [pl.BlockSpec((TILE_ROWS, tile_cols), lambda m, n: (first + m, 0))] * len(out_shape)
    else:
        y_shape, rhs_idx, start = out
        out_shape = jax.ShapeDtypeStruct(y_shape, jnp.bfloat16)
        out_spec = pl.BlockSpec((1, TILE_ROWS, tile_cols), lambda m, n: (rhs_idx, first + m, start // tile_cols + n))
    plan = (tuple(tiles), tuple(flips), tuple(windows), k_start, k_rows, base is not None, len(prevs), width, tile_cols)
    tile_rows = len(tiles) * TILE_ROWS
    vmem = vmem or 4 * n_layers * k_rows * (tile_rows + width) + 16 * TILE_ROWS * tile_cols + (8 << 20)
    return pl.pallas_call(
        functools.partial(product_kernel, plan),
        grid=(len(tiles), width // tile_cols),
        out_shape=out_shape,
        in_specs=in_specs,
        out_specs=out_spec,
        scratch_shapes=[
            pltpu.VMEM((2, tile_rows, n_layers * k_rows), jnp.bfloat16),
            pltpu.VMEM((2 * n_layers, k_rows, width), jnp.bfloat16),
            pltpu.SemaphoreType.DMA((2, len(tiles))),
            pltpu.SemaphoreType.DMA((2 * n_layers, width // tile_cols)),
        ],
        input_output_aliases=aliases,
        cost_estimate=pl.CostEstimate(flops=4 * tile_rows * n_layers * k_rows * width, bytes_accessed=4 * tile_rows * half, transcendentals=0),
        compiler_params=pltpu.CompilerParams(dimension_semantics=("arbitrary", "arbitrary"), vmem_limit_bytes=vmem),
        name="product",
    )(*operands)


def weight_kernel(layer_flip, *refs):
    a_own, a_far, out_ref, sems = refs[0], refs[1:-2], refs[-2], refs[-1]
    slice_rows = out_ref.shape[2]
    start = pl.multiple_of(lax.rem(lax.axis_index("depth") + layer_flip, 2) * slice_rows, slice_rows)
    copies = [pltpu.make_async_copy(a_own.at[:, pl.ds(start, slice_rows)], out_ref.at[0], sems.at[0])]
    for tile, ref in enumerate(a_far):
        block = out_ref.at[1, pl.ds(tile * TILE_ROWS, TILE_ROWS)]
        copies.append(pltpu.make_async_copy(ref.at[:, pl.ds(start, slice_rows)], block, sems.at[tile + 1]))
    for copy in copies:
        copy.start()
    for copy in copies:
        copy.wait()


def late_weights(a_own, a_far):
    rows, half = a_own.shape
    any_spec = pl.BlockSpec(memory_space=pl.ANY)
    return pl.pallas_call(
        functools.partial(weight_kernel, 1),
        out_shape=jax.ShapeDtypeStruct((2, rows, half // 2), jnp.bfloat16),
        in_specs=[pl.BlockSpec(memory_space=pltpu.HBM)] * (1 + len(a_far)),
        out_specs=pl.BlockSpec(memory_space=pltpu.VMEM),
        scratch_shapes=[pltpu.SemaphoreType.DMA((1 + len(a_far),))],
        cost_estimate=pl.CostEstimate(flops=2 * rows * half * 256, bytes_accessed=4 * rows * half, transcendentals=0),
        compiler_params=pltpu.CompilerParams(vmem_limit_bytes=16 << 20),
        name="late_weights",
    )(a_own, *a_far)


def late_kernel(k_start, base_start, target, flips, tile_rows, *refs):
    n_pieces = len(flips)
    weights, pieces, base = refs[0], refs[1 : 1 + n_pieces], refs[1 + n_pieces]
    rest = refs[2 + n_pieces :]
    k_rows, width = pieces[0].shape
    cross = lax.rem(lax.axis_index("col") + lax.axis_index("row"), 2)
    k_range = pl.ds(k_start, k_rows)
    unrolled = isinstance(tile_rows, tuple)
    tiles = len(tile_rows) if unrolled else weights.shape[1] // tile_rows

    def rows_of(tile):
        if unrolled:
            return pl.ds(sum(tile_rows[:tile]), tile_rows[tile])
        return pl.ds(pl.multiple_of(tile * tile_rows, tile_rows), tile_rows)

    def out_copy(tile):
        y_ref, stage, sems = rest[1:]
        rhs_idx, start = target
        return pltpu.make_async_copy(stage.at[rows_of(tile)], y_ref.at[rhs_idx, rows_of(tile), pl.ds(start, width)], sems.at[tile])

    def row_tile(tile, carry):
        row_range = rows_of(tile)
        total = base[row_range, pl.ds(base_start, width)]
        for flip, piece in zip(flips, pieces):
            side = lax.rem(cross + flip, 2)
            total = total + jnp.dot(weights[side, row_range, k_range], piece[...], preferred_element_type=jnp.float32)
        if target is None:
            rest[0][row_range] = total
        else:
            stage = rest[2]
            stage[row_range] = total.astype(stage.dtype)
            out_copy(tile).start()
        return carry

    if unrolled:
        for tile in range(tiles):
            row_tile(tile, 0)
    else:
        lax.fori_loop(0, tiles, row_tile, 0)
    if target is not None:
        for tile in range(tiles):
            out_copy(tile).wait()


def late_product(weights, pieces, flips, base, base_start, k_start, prev=None, target=None, tile_rows=TILE_ROWS):
    vmem_spec = pl.BlockSpec(memory_space=pltpu.VMEM)
    any_spec = pl.BlockSpec(memory_space=pl.ANY)
    rows, width = weights.shape[1], pieces[0].shape[1]
    operands = [weights, *pieces, base]
    in_specs = [vmem_spec] * len(operands)
    scratch = []
    aliases = {}
    if target is None:
        out_shape, out_spec = jax.ShapeDtypeStruct((rows, width), jnp.float32), vmem_spec
    else:
        out_shape, out_spec = jax.ShapeDtypeStruct(prev.shape, prev.dtype), any_spec
        aliases = {len(operands): 0}
        operands.append(prev)
        in_specs.append(any_spec)
        scratch = [pltpu.VMEM((rows, width), jnp.bfloat16), pltpu.SemaphoreType.DMA((len(tile_rows) if isinstance(tile_rows, tuple) else rows // tile_rows,))]
    return pl.pallas_call(
        functools.partial(late_kernel, k_start, base_start, target, flips, tile_rows),
        out_shape=out_shape,
        in_specs=in_specs,
        out_specs=out_spec,
        scratch_shapes=scratch,
        input_output_aliases=aliases,
        name="late",
        compiler_params=pltpu.CompilerParams(vmem_limit_bytes=28 << 20),
        cost_estimate=pl.CostEstimate(flops=2 * rows * len(pieces) * pieces[0].size, bytes_accessed=4 * pieces[0].size, transcendentals=0),
    )(*operands)


OWN, DEEP, PEER, BOTH = (0, 0), (0, 1), (1, 0), (1, 1)


def solution(mesh):
    def permute(value, axis):
        return lax.ppermute(value, axis, SWAP)

    def body(w_local, x_local):
        y_shape = x_local.shape
        slice_rows = y_shape[1]
        n_row_tiles = w_local.shape[0] // TILE_ROWS

        def piece_of(x, chunk):
            rhs_idx, start, width, k_start, k_rows = chunk
            return x[rhs_idx, k_start : k_start + k_rows, start : start + width]

        sends = {SEND_ORDER[0]: piece_of(x_local, CHUNKS[SEND_ORDER[0]])}
        sends[SEND_ORDER[0]], x_rest = lax.optimization_barrier((sends[SEND_ORDER[0]], x_local))
        second = piece_of(x_rest, CHUNKS[SEND_ORDER[1]])
        sends[SEND_ORDER[1]], x_rest, w_rest = lax.optimization_barrier((second, x_rest, w_local))
        w_first, x_rest, w_rest = lax.optimization_barrier((w_rest[:TILE_ROWS], x_rest, w_rest))
        for name in SEND_ORDER[2:]:
            sends[name] = piece_of(x_rest, CHUNKS[name])
        deep = {name: permute(sends[name], "depth") for name in SEND_ORDER}
        w_sends = [w_first] + [w_rest[tile * TILE_ROWS : (tile + 1) * TILE_ROWS] for tile in range(1, n_row_tiles)]
        w_far = [permute(piece, "col") for piece in w_sends]
        x_row = permute(x_rest, "row")

        def full(name, relay, y, tiles):
            rhs_idx, start, width, _, _ = CHUNKS[name]
            window = (rhs_idx, start)
            return product(w_local, w_far, (x_local, deep[name], x_row, relay), (OWN, DEEP, PEER, BOTH), (window, None, window, None), (0, slice_rows), width, tiles=tiles, prev=y, out=(y_shape, rhs_idx, start))

        def local(y, tiles, prev=None):
            rhs_idx, start, width = LATE_COLS
            gated, y = lax.optimization_barrier((x_row, y))
            window = (rhs_idx, start)
            base = product(w_local, w_far, (x_local, gated), (OWN, PEER), (window, window), (0, slice_rows), width, tiles=tiles, prev=prev, vmem=LOCAL_VMEM)
            return lax.optimization_barrier((y, base))

        def relay_after(y, name):
            piece, y = lax.optimization_barrier((deep[name], y))
            return piece, permute(piece, "row"), y

        relay_j0 = permute(deep["j0"], "row")
        relay_a = permute(deep["a"], "row")
        y = full("a", relay_a, None, (0,))
        y, base = local(y, (0,))
        y = full("a", relay_a, y, (1,))
        _, relay, y = relay_after(y, "b")
        y = full("b", relay, y, (0, 1))
        y, base = local(y, (1,), prev=base)
        y = full("a", relay_a, y, (2,))
        y = full("b", relay, y, (2,))
        for name in ("c", "d"):
            _, relay, y = relay_after(y, name)
            y = full(name, relay, y, (0, 1, 2))
        early_i0, relay_i0, y = relay_after(y, "i0")
        early_j1, relay_j1, y = relay_after(y, "j1")
        y, base = local(y, (2,), prev=base)
        w_gate, y = lax.optimization_barrier((w_local, y))
        weights = late_weights(w_gate, w_far)
        y, weights = lax.optimization_barrier((y, weights))

        def base_of(name):
            _, start, _, _, _ = CHUNKS[name]
            return base[start // TILE_COLS], start % TILE_COLS

        def late(name, y):
            piece, relay, y = relay_after(y, name)
            rhs_idx, start, _, k_start, _ = CHUNKS[name]
            return late_product(weights, (piece, relay), (0, 1), *base_of(name), k_start, prev=y, target=(rhs_idx, start))

        def early_part(name, piece, relay, part, part_start):
            return late_product(weights, (piece, relay), (0, 1), part, part_start, CHUNKS[name][3])

        def split_late(name, y, part, part_start, tile_rows=TILE_ROWS):
            piece, relay, y = relay_after(y, name)
            rhs_idx, start, _, k_start, _ = CHUNKS[name]
            part = late_product(weights, (piece,), (0,), part, part_start, k_start, tile_rows=tile_rows)
            return late_product(weights, (relay,), (1,), part, 0, k_start, prev=y, target=(rhs_idx, start), tile_rows=(256,) * 6 if tile_rows == SMALL_ROWS else tile_rows)

        part_j = early_part("j0", deep["j0"], relay_j0, *base_of("j0"))
        y, part_j = lax.optimization_barrier((y, part_j))
        y = late("e", y)
        part_i = early_part("i0", early_i0, relay_i0, *base_of("i0"))
        part_j = early_part("j1", early_j1, relay_j1, part_j, 0)
        y, part_i, part_j = lax.optimization_barrier((y, part_i, part_j))
        y = late("f", y)
        x_gate, y = lax.optimization_barrier((x_local, y))
        for name in SENT_LATE:
            deep[name] = permute(piece_of(x_gate, CHUNKS[name]), "depth")
        for name in ("g", "h"):
            y = split_late(name, y, *base_of(name))
        y = split_late("i1", y, part_i, 0, SMALL_ROWS)
        return split_late("j2", y, part_j, 0, SMALL_ROWS)

    return jax.shard_map(body, mesh=mesh, in_specs=(P(("row", "depth"), "col"), P(None, ("row", "depth"), "col")), out_specs=P(None, ("row", "depth"), "col"), check_vma=False)
```
